32 devices in a mesh: blk: 32 (over z, y, x, core).
Axes of the slice: x: 2, y: 2, z: 4, core: 2. Of those that a mesh axis runs over, the one named last changes fastest.
Arguments:
- image_features: bfloat16 [8192, 1536], P('blk'), may hold values from -0.119628906 to 0.119628906
- head_weight: bfloat16 [1536, 1152], P('blk'), may hold values from -0.15625 to 0.15625
- text_embeds: bfloat16 [8192, 1152], P('blk'), may hold values from -0.29882812 to 0.29882812
- natural_exponent_factor: float32 [1], replicated, may hold values from 1.6 to 2.6
- logit_bias: float32 [1], replicated, may hold values from -4 to -1
Outputs:
- grad_features: bfloat16 [8192, 1536], P('blk')
- grad_text: bfloat16 [8192, 1152], P('blk')
- grad_weight: float32 [1536, 1152], P('blk')
The draws below stay inside these ranges and needn't reach their ends.
All inputs are finite; a program needn't handle non-finite values.
Results may differ from the reference program's by a relative error of at most 0.0085.
Values may be sent and summed in bfloat16 or wider, within the bound.
A program may use at most 64 MiB of HBM per device.

```python
import jax
import jax.numpy as jnp
from jax import lax

D = 1536
E = 1152
R = 256
S = 4
TOTAL = 8192
N_BLK = 32


def strengthened(entries, rng, source, target, blocks, factor):
    owner, partner = [(jnp.arange(entries.shape[axis_at]) // (entries.shape[axis_at] // blocks)).reshape([-1 if axis == axis_at else 1 for axis in range(entries.ndim)]) for axis_at in (source, target)]
    chosen = jax.random.permutation(rng, blocks)[partner]
    strong = (owner == chosen) | (owner == (partner + blocks // 2) % blocks)
    return jnp.where(strong, factor * entries, entries)


def levels(rng, extent, split, least, largest):
    def one(position, parts):
        steps = jax.random.uniform(jax.random.fold_in(jax.random.fold_in(rng, 6), position), (parts,), jnp.float32, least / len(split), largest / len(split))
        return jnp.repeat(jnp.exp(steps), extent[position] // parts).reshape((-1,) + (1,) * (len(extent) - position - 1))

    level = one(*split[0])
    for cut in split[1:]:
        level = level * one(*cut)
    return level


def bell_draw(stream_key, dims, scale, bound, pieces=(), kind=jnp.bfloat16):
    drawn = jax.random.normal(stream_key, dims, jnp.float32) * scale
    if len(pieces) > 0:
        drawn = levels(stream_key, dims, pieces, -0.22, 0.18) * drawn
    return jnp.clip(drawn, min=-bound, max=bound).astype(kind)


def heavy_noise(key, shape, spread, reach, pieces, heavy, kind=jnp.bfloat16):
    drawn = spread * jax.random.normal(key, shape, jnp.float32)
    if pieces:
        drawn = drawn * levels(key, shape, pieces, -0.22, 0.18)
    return jnp.clip(strengthened(drawn, jax.random.fold_in(key, 3), *heavy), -reach, reach).astype(kind)


def setup_inputs(seed: int = 0) -> dict:
    streams_of = jax.random.split(jax.random.key(seed), 6)
    return {
        "image_features": heavy_noise(streams_of[0], (TOTAL, D), 0.02, 0.119628906, ((0, 32),), (0, 1, 32, 2.75)),
        "head_weight": bell_draw(streams_of[1], (D, E), D ** -0.5, 0.15625, ((0, 32),)),
        "text_embeds": bell_draw(streams_of[2], (TOTAL, E), 0.05, 0.29882812, ((0, 32),)),
        "natural_exponent_factor": jnp.clip(jax.random.uniform(streams_of[3], (1,), jnp.float32, 1.6, 2.6), 1.6, 2.6),
        "logit_bias": jnp.clip(jax.random.uniform(streams_of[4], (1,), jnp.float32, -4.0, -1.0), -4.0, -1.0),
    }


epsilon = 1e-06

def normalize(rows):
    squares = lax.optimization_barrier(jnp.sum(rows * rows, axis=1, keepdims=True))
    length = jnp.sqrt(squares + epsilon)
    return (rows / length, length)

def similarity_derivative(picture_sample_group, caption_sample_group, similarity_multiplier, neighbour_distance, outer_dimension_size):
    similarity_matrix = similarity_multiplier * lax.dot_general(picture_sample_group, caption_sample_group, (((1,), (1,)), ((), ())), preferred_element_type=jnp.float32) + neighbour_distance
    if outer_dimension_size:
        matched = lax.broadcasted_iota(jnp.int32, similarity_matrix.shape, 0) == lax.broadcasted_iota(jnp.int32, similarity_matrix.shape, 1)
        match_polarity = jnp.where(matched, 1.0, -1.0).astype(jnp.float32)
    else:
        match_polarity = -jnp.ones(similarity_matrix.shape, jnp.float32)
    return (-similarity_multiplier * match_polarity * jax.nn.sigmoid(-match_polarity * similarity_matrix)).astype(jnp.bfloat16)

def project_back(grad, unit_rows, length):
    return (grad - unit_rows * lax.optimization_barrier(jnp.sum(unit_rows * grad, axis=1, keepdims=True))) / length

def reference(image_features, head_weight, text_embeds, natural_exponent_factor, logit_bias):
    embedded = jnp.dot(image_features, head_weight, preferred_element_type=jnp.float32)
    image_unit, image_length = normalize(embedded)
    picture_embedding_mapped = image_unit.astype(jnp.bfloat16)
    text_unit, text_length = normalize(text_embeds.astype(jnp.float32))
    text_low = text_unit.astype(jnp.bfloat16)
    similarity_multiplier = jnp.exp(natural_exponent_factor[0])
    neighbour_distance = logit_bias[0]
    image_blocks = picture_embedding_mapped.reshape(N_BLK, R, E)
    text_blocks = text_low.reshape(N_BLK, R, E)

    def pick_block(blocks, block_id):
        where_at = ((block_id + N_BLK) % N_BLK).astype(jnp.int32)
        return lax.dynamic_index_in_dim(blocks, where_at, 0, keepdims=False)

    def image_side(block_id):
        picture_sample_group = pick_block(image_blocks, block_id)
        summed = jnp.zeros((R, E), jnp.float32)
        for partition_portion in range(S):
            caption_sample_group = pick_block(text_blocks, block_id + partition_portion)
            mapping_matrix = similarity_derivative(picture_sample_group, caption_sample_group, similarity_multiplier, neighbour_distance, partition_portion == 0)
            summed = summed + jnp.dot(mapping_matrix, caption_sample_group, preferred_element_type=jnp.float32)
        return summed

    def text_side(block_id):
        caption_sample_group = pick_block(text_blocks, block_id)
        summed = jnp.zeros((R, E), jnp.float32)
        for partition_portion in range(S):
            picture_sample_group = pick_block(image_blocks, block_id - partition_portion)
            mapping_matrix = similarity_derivative(picture_sample_group, caption_sample_group, similarity_multiplier, neighbour_distance, partition_portion == 0)
            summed = summed + lax.dot_general(mapping_matrix, picture_sample_group, (((0,), (0,)), ((), ())), preferred_element_type=jnp.float32)
        return summed
    block_ids = jnp.arange(N_BLK, dtype=jnp.int32)
    image_grad = lax.map(image_side, block_ids).reshape(-1, E)
    text_grad = lax.map(text_side, block_ids).reshape(-1, E)
    embed_grad = project_back(image_grad, image_unit, image_length).astype(jnp.bfloat16)
    grad_text = project_back(text_grad, text_unit, text_length).astype(jnp.bfloat16)
    grad_features = lax.dot_general(embed_grad, head_weight, (((1,), (1,)), ((), ())), preferred_element_type=jnp.float32).astype(jnp.bfloat16)
    grad_weight = lax.dot_general(image_features, embed_grad, (((0,), (0,)), ((), ())), preferred_element_type=jnp.float32)
    return (grad_features, grad_text, grad_weight)
```

```python
import functools

import jax
import jax.numpy as jnp
from jax import lax
from jax.experimental import pallas as pl
from jax.experimental.pallas import tpu as pltpu
from jax.sharding import PartitionSpec as P

S = 4
epsilon = 1e-06
MESH = pl.DeviceIdType.MESH
F32 = jnp.float32
BF = jnp.bfloat16


def dot_nt(a, b):
    return lax.dot_general(a, b, (((1,), (1,)), ((), ())), preferred_element_type=F32)


def pair_grad(rows, cols, t, bias, own):
    logits = t * dot_nt(rows, cols) + bias
    if own:
        matched = lax.broadcasted_iota(jnp.int32, logits.shape, 0) == lax.broadcasted_iota(
            jnp.int32, logits.shape, 1
        )
        z = jnp.where(matched, 1.0, -1.0).astype(F32)
        return (-t * z * jax.nn.sigmoid(-z * logits)).astype(BF)
    return (t * jax.nn.sigmoid(logits)).astype(BF)


CHUNKS = 4


def sem_keys():
    keys = ["o1", "o2", "o3", "s2", "s3", "rx", "ry"]
    for p in range(4):
        keys += [("px", p), ("py", p), ("dA", p), ("dB", p), ("zx", p), ("zy", p)]
        keys += [("w", p, i) for i in range(5)]
        keys += [("g0", p), ("gA", p), ("gB", p)]
    keys += ["g1o", "g2o", "g3o", "gs2", "gs3", "gx3", "gy3", "gx0", "gy0"]
    keys += ["g1x", "g1y", "gex", "gey", "g2x", "g2y"]
    for k in ("t", "i"):
        keys += [(k, "own")]
        for kind in ("near", "far", "pass", "first", "second", "relay", "relay2", "onear", "ofar"):
            keys += [(k, kind, c) for c in range(CHUNKS)]
    return {k: i for i, k in enumerate(keys)}


def kernel(
    n, axis, keys,
    x_hbm, w_hbm, t_hbm, lf_hbm, bias_hbm,
    gx_ref, gt_ref, gw_ref,
    x_ref, t_ref, w_all, text_low, text_in, image_low, image_in, xt, gz, from_core, to_core,
    out_s, in_d, in_xy, in_z, in_e,
    factor_ref, bias_ref, load_sem, send_sem, recv_sem,
):
    rows, width = x_ref.shape
    own_rows, cols = w_all.shape[1:]
    ha = (cols // 128 + 1) // 2 * 128
    A, B, FULL = pl.ds(0, ha), pl.ds(ha, cols - ha), pl.ds(0, cols)
    me = lax.axis_index(axis)
    core = lax.rem(me, 2)
    chip = me // 2
    x = lax.rem(chip, 2)
    y = lax.rem(chip // 2, 2)
    z = chip // 4
    side = z // 2
    plane = [z, z + 1 - 2 * lax.rem(z, 2), 2 - side, 3 * (1 - side)]
    inner = lax.rem(z + side, 2) == 1
    outer = jnp.logical_not(inner)
    other = 1 - core

    def dev(z_, y_, x_, c_):
        return ((z_ * 2 + y_) * 2 + x_) * 2 + c_

    xn, yn, partner = dev(z, y, 1 - x, core), dev(z, 1 - y, x, core), dev(z, y, x, other)
    peer = [None] + [dev(plane[p], y, x, core) for p in range(1, 4)]

    def place(r):
        return (y, 1 - y)[r in ("y", "d")], (x, 1 - x)[r in ("x", "d")]

    def shard(p, r, c_=None):
        y_, x_ = place(r)
        return dev(plane[p], y_, x_, core if c_ is None else c_)

    waits = []

    def copy(src, dst, key, target, recv=None):
        i = keys[key]
        return pltpu.make_async_remote_copy(
            src_ref=src, dst_ref=dst, send_sem=send_sem.at[i],
            recv_sem=recv_sem.at[i if recv is None else recv],
            device_id=(target,), device_id_type=MESH,
        )

    def send(src, dst, key, target, recv=None, cond=None):
        c = copy(src, dst, key, target, recv)
        if cond is None:
            c.start()
        else:
            pl.when(cond)(c.start)
        waits.append((cond, c))

    def arrived(dst, key):
        copy(dst, dst, key, partner).wait_recv()

    barrier = pltpu.get_barrier_semaphore()
    peers = [partner, xn, yn] + peer[1:] + [lax.rem(me + n + s, n) for s in (-2, 2, -4, 4)]
    for p in peers:
        pl.semaphore_signal(barrier, inc=1, device_id=(p,), device_id_type=MESH)

    loads = [
        pltpu.make_async_copy(src, dst, load_sem.at[i])
        for i, (src, dst) in enumerate(
            [
                (w_hbm, w_all.at[me]), (t_hbm, t_ref), (lf_hbm, factor_ref), (bias_hbm, bias_ref),
                (x_hbm, x_ref),
            ]
        )
    ]
    for c in loads:
        c.start()
    for c in loads[1:4]:
        c.wait()
    t = jnp.exp(jnp.full((1, 1), factor_ref[0], F32))
    bias = bias_ref[0]
    text = t_ref[...].astype(F32)
    text_length = jnp.sqrt(jnp.sum(text * text, axis=1, keepdims=True) + epsilon)
    text_low[...] = (text / text_length).astype(BF)
    loads[0].wait()

    pl.semaphore_wait(barrier, len(peers))

    def w_at(p, r, cut=FULL):
        return w_all.at[shard(p, r), :, cut]

    def swap(p, r, i, cut=FULL):
        send(w_at(p, r, cut), w_at(p, r, cut), ("w", p, i), partner)

    def onto(p, r, cut, key, target, cond=None, dst_key=None):
        send(w_at(p, r, cut), w_at(p, r, cut), key, target, None if dst_key is None else keys[dst_key], cond)

    far_key = jnp.where(inner, keys["o2"], keys["o3"])
    own = w_all.at[me]
    send(own, own, "s3", peer[3], far_key)
    send(own, own, "s2", peer[2], far_key)
    send(own, own, "o1", peer[1])
    send(own, own, ("px", 0), xn)
    send(own, own, ("py", 0), yn)
    send(own, own, ("w", 0, 0), partner)

    part = rows // CHUNKS

    class Window:
        def __init__(self, key, buf, slots, mirror):
            self.key, self.buf, self.slots = key, buf, slots
            v = n - 1 - me if mirror else me
            self.c = lax.rem(v, 2)
            q = lax.rem(v // 2, 4)
            self.q = q
            step = 2 if mirror else -2
            back = lax.rem(me + n + step, n)
            back2 = lax.rem(me + n + 2 * step, n)
            back4 = lax.rem(me + n + 4 * step, n)
            first_c = self.c == 0
            odd = lax.rem(q, 2) == 1
            even = jnp.logical_not(odd)
            far_first = jnp.logical_and(first_c, even)
            self.first_target = jnp.where(far_first, back2, back)
            self.first_slot = jnp.where(far_first, 3, self.c)
            self.first_kind = jnp.where(far_first, 1, 0)
            self.is_c0 = first_c
            self.is_c1 = jnp.logical_not(first_c)
            self.has_second = jnp.logical_and(first_c, odd)
            passing = q == 1
            self.second_target = jnp.where(passing, back4, back2)
            self.second_slot = jnp.where(passing, 4, 3)
            self.second_kind = jnp.where(passing, 2, 1)
            self.relays = far_first
            self.passes = jnp.logical_and(first_c, passing)

        def rows(self, c):
            return pl.ds(c * part, part)

        def recv(self, kind, c):
            return keys[(self.key, "near", c)] + CHUNKS * kind

        def start(self, c):
            r = self.rows(c)
            send(
                self.buf.at[r], self.slots.at[self.first_slot, r], (self.key, "first", c),
                self.first_target, self.recv(self.first_kind, c),
            )
            send(
                self.buf.at[r], self.slots.at[self.second_slot, r], (self.key, "second", c),
                self.second_target, self.recv(self.second_kind, c), self.has_second,
            )

        def own(self):
            send(self.buf, self.slots.at[2], (self.key, "own"), partner, None, self.is_c1)

        def passed(self, c):
            r = self.rows(c)

            @pl.when(self.passes)
            def _():
                arrived(self.slots.at[4, r], (self.key, "pass", c))

            send(
                self.slots.at[4, r], self.slots.at[3, r], (self.key, "relay2", c), yn,
                self.recv(1, c), self.passes,
            )

        def far(self, c):
            r = self.rows(c)

            @pl.when(self.is_c0)
            def _():
                arrived(self.slots.at[3, r], (self.key, "far", c))

            send(
                self.slots.at[3, r], self.slots.at[0, r], (self.key, "relay", c), xn,
                self.recv(0, c), self.relays,
            )
            send(
                self.slots.at[3, r], self.slots.at[2, r], (self.key, "ofar", c), partner,
                None, self.is_c0,
            )

        def near(self, c):
            r = self.rows(c)
            slot = self.slots.at[self.c, r]
            arrived(slot, (self.key, "near", c))
            send(slot, slot, (self.key, "onear", c), partner)

        def wait_near_partner(self):
            for c in range(CHUNKS):
                arrived(self.slots.at[1 - self.c, self.rows(c)], (self.key, "onear", c))

        def wait_last(self):
            @pl.when(self.is_c0)
            def _():
                arrived(self.slots.at[2], (self.key, "own"))

            @pl.when(self.is_c1)
            def _():
                for c in range(CHUNKS):
                    arrived(self.slots.at[2, self.rows(c)], (self.key, "ofar", c))

    tw = Window("t", text_low, text_in, False)
    iw = Window("i", image_low, image_in, True)

    def got_plane(p):
        arrived(w_at(p, "d", A), ("dA", p))
        swap(p, "d", 3, A)
        arrived(w_at(p, "d", B), ("dB", p))
        swap(p, "d", 4, B)

    def side_x(p, key):
        arrived(w_at(p, "x"), key)
        onto(p, "x", A, ("dA", p), yn)

    def side_y(p, key):
        arrived(w_at(p, "y"), key)
        onto(p, "y", B, ("dB", p), xn)

    tw.own()
    tw.start(0)
    side_x(0, ("px", 0))
    onto(0, "x", FULL, ("zx", 1), peer[1])
    onto(0, "x", FULL, ("zx", 2), peer[2], inner)
    swap(0, "x", 1)
    side_y(0, ("py", 0))
    onto(0, "y", FULL, ("zy", 1), peer[1])
    onto(0, "y", FULL, ("zy", 2), peer[2], inner)
    swap(0, "y", 2)
    tw.start(1)
    arrived(w_at(3, "o"), "o3")
    onto(3, "o", FULL, ("px", 3), xn)
    onto(3, "o", FULL, ("py", 3), yn)
    tw.start(2)
    swap(3, "o", 0)
    arrived(w_at(1, "o"), "o1")
    swap(1, "o", 0)
    arrived(w_at(2, "o"), "o2")
    swap(2, "o", 0)
    got_plane(0)
    tw.passed(0)
    tw.far(0)
    tw.start(3)
    side_x(1, ("zx", 1))
    swap(1, "x", 1)
    side_y(1, ("zy", 1))
    swap(1, "y", 2)
    tw.passed(1)
    tw.far(1)
    side_x(3, ("px", 3))
    swap(3, "x", 1)
    side_y(3, ("py", 3))
    swap(3, "y", 2)
    tw.passed(2)
    tw.far(2)
    side_x(2, ("zx", 2))
    onto(2, "x", FULL, "rx", peer[1], inner, ("zx", 2))
    swap(2, "x", 1)
    side_y(2, ("zy", 2))
    onto(2, "y", FULL, "ry", peer[1], inner, ("zy", 2))
    swap(2, "y", 2)
    got_plane(1)
    got_plane(3)
    tw.passed(3)
    tw.far(3)
    got_plane(2)
    loads[4].wait()
    xt[...] = x_ref[...].T

    for p in range(4):
        for i, (r, cut) in enumerate([("o", FULL), ("x", FULL), ("y", FULL), ("d", A), ("d", B)]):
            arrived(w_all.at[shard(p, r, other), :, cut], ("w", p, i))

    weight = w_all[...].reshape(n * own_rows, cols)
    embedded = jnp.dot(x_ref[...], weight, preferred_element_type=F32)
    image_length = jnp.sqrt(jnp.sum(embedded * embedded, axis=1, keepdims=True) + epsilon)
    image_unit = embedded / image_length
    image_low[...] = image_unit.astype(BF)
    iw.own()
    for c in range(CHUNKS):
        iw.start(c)
    mine = image_low[...]
    own_text = text_low[...]
    grad = pair_grad(mine, own_text, t, bias, True)
    image_grad = jnp.dot(grad, own_text, preferred_element_type=F32)

    for c in range(CHUNKS):
        tw.near(c)

    def window(low, win, grads):
        for q in (2, 0, 1):
            if q == 2:
                win.wait_last()
            if q == 0:
                win.wait_near_partner()
            block = win.slots[q]
            grads += jnp.dot(
                pair_grad(low, block, t, bias, False), block, preferred_element_type=F32
            )
        return grads

    image_grad = window(mine, tw, image_grad)
    iw.passed(0)
    iw.far(0)
    along = jnp.sum(image_unit * image_grad, axis=1, keepdims=True)
    embed_grad = ((image_grad - image_unit * along) / image_length).astype(BF)

    def spot(p, r):
        y_, x_ = place(r)
        return y_ * 2 + x_

    group = 8 * own_rows
    for p in (3, 2, 1, 0):
        lhs = xt[pl.ds(pl.multiple_of(plane[p] * group, group), group), :]
        product = jnp.dot(lhs, embed_grad, preferred_element_type=F32)
        gz[p] = product.reshape(4, 2, own_rows, cols)
        for c in range(4):
            to_core[p, c] = gz[p, c, other].astype(BF)
        send(to_core.at[p], from_core.at[p], ("g0", p), partner)

    S_O, S_X, S_Y, S_D = range(4)

    def base(p, r, cut):
        c = spot(p, r)
        return gz[p, c, core, :, cut] + from_core[p, c, :, cut].astype(F32)

    def put(p, r, cut, value):
        out_s[p, r, :, cut] = value.astype(BF)

    def open_plane(p):
        arrived(from_core.at[p], ("g0", p))
        put(p, S_D, FULL, base(p, "d", FULL))
        send(out_s.at[p, S_D, :, A], in_d.at[p, :, A], ("gA", p), yn)
        send(out_s.at[p, S_D, :, B], in_d.at[p, :, B], ("gB", p), xn)

    gs_key = jnp.where(inner, keys["g2o"], keys["g3o"])
    gs_slot = jnp.where(inner, 1, 2)

    def sides(p):
        arrived(in_d.at[p, :, A], ("gA", p))
        arrived(in_d.at[p, :, B], ("gB", p))

    def x_sum(p, cut):
        v = base(p, "x", cut)
        return v + in_d[p, :, cut].astype(F32) if cut is A else v

    def y_sum(p, cut):
        v = base(p, "y", cut)
        return v + in_d[p, :, cut].astype(F32) if cut is B else v

    open_plane(3)
    open_plane(2)
    iw.passed(1)
    iw.far(1)
    put(2, S_O, FULL, base(2, "o", FULL))
    send(out_s.at[2, S_O], in_z.at[gs_slot, 0], "gs2", peer[2], gs_key)
    open_plane(1)
    iw.passed(2)
    iw.far(2)
    put(1, S_O, FULL, base(1, "o", FULL))
    send(out_s.at[1, S_O], in_z.at[0, 0], "g1o", peer[1])
    sides(3)
    for cut in (A, B):
        put(3, S_X, cut, x_sum(3, cut))
        put(3, S_Y, cut, y_sum(3, cut))
    send(out_s.at[3, S_X], in_xy.at[1, 0], "gx3", xn)
    send(out_s.at[3, S_Y], in_xy.at[1, 1], "gy3", yn)
    iw.passed(3)
    iw.far(3)
    open_plane(0)
    sides(2)
    for cut in (A, B):
        put(2, S_X, cut, x_sum(2, cut))
        put(2, S_Y, cut, y_sum(2, cut))

    @pl.when(outer)
    def _():
        copy(out_s.at[2, S_X], in_e.at[0], "gex", peer[1]).start()
        copy(out_s.at[2, S_Y], in_e.at[1], "gey", peer[1]).start()

    sides(1)
    for cut in (A, B):
        put(1, S_X, cut, x_sum(1, cut))
        put(1, S_Y, cut, y_sum(1, cut))
    send(out_s.at[1, S_X], in_z.at[0, 1], "g1x", peer[1])
    send(out_s.at[1, S_Y], in_z.at[0, 2], "g1y", peer[1])

    gx_ref[...] = dot_nt(embed_grad, weight).astype(BF)

    @pl.when(inner)
    def _():
        for r, key, fill in ((S_X, "gex", x_sum), (S_Y, "gey", y_sum)):
            arrived(in_e.at[r - 1], key)
            for cut in (A, B):
                put(2, r, cut, fill(2, cut) + in_e[r - 1, :, cut].astype(F32))
            copy(out_s.at[2, r], in_z.at[1, r], ("g2x", "g2y")[r - 1], peer[2]).start()

    arrived(in_xy.at[1, 0], "gx3")
    arrived(in_xy.at[1, 1], "gy3")
    put(
        3, S_O, FULL,
        base(3, "o", FULL) + in_xy[1, 0].astype(F32) + in_xy[1, 1].astype(F32),
    )
    send(out_s.at[3, S_O], in_z.at[gs_slot, 0], "gs3", peer[3], gs_key)

    text_grad = jnp.dot(
        pair_grad(own_text, mine, t, bias, True), mine, preferred_element_type=F32
    )
    for c in range(CHUNKS):
        iw.near(c)

    sides(0)
    arrived(in_z.at[0, 1], "g1x")
    arrived(in_z.at[0, 2], "g1y")

    @pl.when(outer)
    def _():
        for cut in (A, B):
            put(0, S_X, cut, x_sum(0, cut) + in_z[0, 1, :, cut].astype(F32))
            put(0, S_Y, cut, y_sum(0, cut) + in_z[0, 2, :, cut].astype(F32))

    @pl.when(inner)
    def _():
        arrived(in_z.at[1, 1], "g2x")
        arrived(in_z.at[1, 2], "g2y")
        for cut in (A, B):
            for r, fill in ((1, x_sum), (2, y_sum)):
                put(
                    0, r, cut,
                    fill(0, cut) + in_z[0, r, :, cut].astype(F32) + in_z[1, r, :, cut].astype(F32),
                )

    send(out_s.at[0, S_X], in_xy.at[0, 0], "gx0", xn)
    send(out_s.at[0, S_Y], in_xy.at[0, 1], "gy0", yn)

    text_grad = window(own_text, iw, text_grad)
    text_unit = t_ref[...].astype(F32) / text_length
    along = jnp.sum(text_unit * text_grad, axis=1, keepdims=True)
    gt_ref[...] = ((text_grad - text_unit * along) / text_length).astype(BF)

    total = base(0, "o", FULL)
    for i, key in enumerate(("g1o", "g2o", "g3o")):
        arrived(in_z.at[i, 0], key)
        total += in_z[i, 0].astype(F32)
    gw_ref[...] = total
    arrived(in_xy.at[0, 0], "gx0")
    arrived(in_xy.at[0, 1], "gy0")
    gw_ref[...] += in_xy[0, 0].astype(F32) + in_xy[0, 1].astype(F32)

    for cond, c in waits:
        if cond is None:
            c.wait_send()
        else:
            pl.when(cond)(c.wait_send)

    @pl.when(outer)
    def _():
        copy(out_s.at[2, S_X], in_e.at[0], "gex", peer[1]).wait_send()
        copy(out_s.at[2, S_Y], in_e.at[1], "gey", peer[1]).wait_send()

    @pl.when(inner)
    def _():
        copy(out_s.at[2, S_X], in_z.at[1, 1], "g2x", peer[2]).wait_send()
        copy(out_s.at[2, S_Y], in_z.at[1, 2], "g2y", peer[2]).wait_send()


def fused(n, axis, image_features, head_weight, text_embeds, factor, bias):
    rows, width = image_features.shape
    own_rows, cols = head_weight.shape
    keys = sem_keys()
    hbm = pl.BlockSpec(memory_space=pltpu.HBM)
    vmem = pl.BlockSpec(memory_space=pltpu.VMEM)
    scratch = [
        ((rows, width), BF),
        ((rows, cols), BF),
        ((n, own_rows, cols), BF),
        ((rows, cols), BF),
        ((5, rows, cols), BF),
        ((rows, cols), BF),
        ((5, rows, cols), BF),
        ((width, rows), BF),
        ((4, 4, 2, own_rows, cols), F32),
        ((4, 4, own_rows, cols), BF),
        ((4, 4, own_rows, cols), BF),
        ((4, 4, own_rows, cols), BF),
        ((4, own_rows, cols), BF),
        ((2, 2, own_rows, cols), BF),
        ((3, 3, own_rows, cols), BF),
        ((2, own_rows, cols), BF),
    ]
    results = pl.pallas_call(
        functools.partial(kernel, n, axis, keys),
        out_shape=(
            pltpu.VMEM((rows, width), BF),
            pltpu.VMEM((rows, cols), BF),
            pltpu.VMEM((own_rows, cols), F32),
        ),
        in_specs=[hbm] * 5,
        out_specs=(vmem, vmem, vmem),
        scratch_shapes=[pltpu.VMEM(s, d) for s, d in scratch]
        + [pltpu.SMEM((1,), F32)] * 2
        + [pltpu.SemaphoreType.DMA((5,))]
        + [pltpu.SemaphoreType.DMA((len(keys),))] * 2,
        compiler_params=pltpu.CompilerParams(
            collective_id=0, has_side_effects=True, vmem_limit_bytes=65413120
        ),
    )(image_features, head_weight, text_embeds, factor, bias)
    return pl.pallas_call(
        write_out,
        out_shape=(
            jax.ShapeDtypeStruct((rows, width), BF),
            jax.ShapeDtypeStruct((rows, cols), BF),
            jax.ShapeDtypeStruct((own_rows, cols), F32),
        ),
        in_specs=[vmem] * 3,
        out_specs=(hbm,) * 3,
        scratch_shapes=[pltpu.SemaphoreType.DMA((3,))],
        compiler_params=pltpu.CompilerParams(vmem_limit_bytes=2**20),
    )(*results)


def write_out(gx, gt, gw, gx_out, gt_out, gw_out, sems):
    pairs = ((gx, gx_out), (gt, gt_out), (gw, gw_out))
    copies = [pltpu.make_async_copy(a, b, sems.at[i]) for i, (a, b) in enumerate(pairs)]
    for c in copies:
        c.start()
    for c in copies:
        c.wait()


def passed_along(block, axis, distance):
    devices = range(lax.axis_size(axis))
    route = [((i - distance) % len(devices), i) for i in devices]
    return lax.ppermute(block, axis, route)


def normalize(rows):
    squares = jnp.sum(rows * rows, axis=1, keepdims=True)
    length = jnp.sqrt(squares + epsilon)
    return (rows / length, length)


def similarity_derivative(
    picture_sample_group,
    caption_sample_group,
    similarity_multiplier,
    neighbour_distance,
    outer_dimension_size,
):
    similarity_matrix = (
        similarity_multiplier
        * lax.dot_general(
            picture_sample_group,
            caption_sample_group,
            (((1,), (1,)), ((), ())),
            preferred_element_type=jnp.float32,
        )
        + neighbour_distance
    )
    if outer_dimension_size:
        matched = lax.broadcasted_iota(
            jnp.int32, similarity_matrix.shape, 0
        ) == lax.broadcasted_iota(jnp.int32, similarity_matrix.shape, 1)
        match_polarity = jnp.where(matched, 1.0, -1.0).astype(jnp.float32)
    else:
        match_polarity = -jnp.ones(similarity_matrix.shape, jnp.float32)
    return (
        -similarity_multiplier
        * match_polarity
        * jax.nn.sigmoid(-match_polarity * similarity_matrix)
    ).astype(jnp.bfloat16)


def project_back(grad, unit_rows, length):
    return (grad - unit_rows * jnp.sum(unit_rows * grad, axis=1, keepdims=True)) / length


def by_collectives(image_features, head_weight, text_embeds, natural_exponent_factor, logit_bias):
    full_weight = lax.all_gather(head_weight, "blk", axis=0, tiled=True)
    embedded = jnp.dot(image_features, full_weight, preferred_element_type=jnp.float32)
    image_unit, image_length = normalize(embedded)
    picture_embedding_mapped = image_unit.astype(jnp.bfloat16)
    text_unit, text_length = normalize(text_embeds.astype(jnp.float32))
    text_low = text_unit.astype(jnp.bfloat16)
    similarity_multiplier = jnp.exp(natural_exponent_factor[0])
    neighbour_distance = logit_bias[0]
    image_grad = jnp.zeros(image_unit.shape, jnp.float32)
    current_neighbour_tile = text_low
    for partition_portion in range(S):
        mapping_matrix = similarity_derivative(
            picture_embedding_mapped,
            current_neighbour_tile,
            similarity_multiplier,
            neighbour_distance,
            partition_portion == 0,
        )
        image_grad = image_grad + jnp.dot(
            mapping_matrix, current_neighbour_tile, preferred_element_type=jnp.float32
        )
        if partition_portion + 1 < S:
            current_neighbour_tile = passed_along(current_neighbour_tile, "blk", -1)
    text_grad = jnp.zeros(text_unit.shape, jnp.float32)
    passing = picture_embedding_mapped
    for partition_portion in range(S):
        mapping_matrix = similarity_derivative(
            passing, text_low, similarity_multiplier, neighbour_distance, partition_portion == 0
        )
        text_grad = text_grad + lax.dot_general(
            mapping_matrix, passing, (((0,), (0,)), ((), ())), preferred_element_type=jnp.float32
        )
        if partition_portion + 1 < S:
            passing = passed_along(passing, "blk", 1)
    embed_grad = project_back(image_grad, image_unit, image_length).astype(jnp.bfloat16)
    grad_text = project_back(text_grad, text_unit, text_length).astype(jnp.bfloat16)
    grad_features = lax.dot_general(
        embed_grad, full_weight, (((1,), (1,)), ((), ())), preferred_element_type=jnp.float32
    ).astype(jnp.bfloat16)
    grad_weight = lax.psum_scatter(
        lax.dot_general(
            image_features, embed_grad, (((0,), (0,)), ((), ())), preferred_element_type=jnp.float32
        ),
        "blk",
        scatter_dimension=0,
        tiled=True,
    )
    return (grad_features, grad_text, grad_weight)


def on_device(image_features, head_weight, text_embeds, natural_exponent_factor, logit_bias):
    n = lax.axis_size("blk")
    whole_tiles = head_weight.shape[0] % 16 == 0 and n % 8 == 0 and n // 8 == 4
    run = functools.partial(fused, n, "blk") if whole_tiles else by_collectives
    return run(image_features, head_weight, text_embeds, natural_exponent_factor, logit_bias)


def solution(mesh):
    return jax.shard_map(
        on_device,
        mesh=mesh,
        in_specs=(P("blk", None), P("blk", None), P("blk", None), P(), P()),
        out_specs=(P("blk", None), P("blk", None), P("blk", None)),
        check_vma=False,
    )
```

```python
import functools

import jax
import jax.numpy as jnp
from jax import lax
from jax.experimental import pallas as pl
from jax.experimental.pallas import tpu as pltpu
from jax.sharding import PartitionSpec as P

S = 4
epsilon = 1e-06
MESH = pl.DeviceIdType.MESH
F32 = jnp.float32
BF = jnp.bfloat16


def dot_nt(a, b):
    return lax.dot_general(a, b, (((1,), (1,)), ((), ())), preferred_element_type=F32)


def pair_grad(rows, cols, t, bias, own):
    logits = t * dot_nt(rows, cols) + bias
    if own:
        matched = lax.broadcasted_iota(jnp.int32, logits.shape, 0) == lax.broadcasted_iota(
            jnp.int32, logits.shape, 1
        )
        z = jnp.where(matched, 1.0, -1.0).astype(F32)
        return (-t * z * jax.nn.sigmoid(-z * logits)).astype(BF)
    return (t * jax.nn.sigmoid(logits)).astype(BF)


CHUNKS = 4
SENDS = 16
RECVS = 48


class Keys(dict):
    def __missing__(self, key):
        self[key] = len(self)
        return self[key]


def kernel(
    n, axis,
    x_hbm, w_hbm, t_hbm, scalars,
    gx_ref, gt_ref, gw_ref,
    x_ref, t_ref, w_all, text_low, text_in, image_low, image_in, xt, gz, from_core, to_core,
    out_s, in_d, in_xy, in_z, in_e, in_fin, pre_out, pre_in, embedded_ref,
    load_sem, send_sem, recv_sem, credit,
):
    rows, width = x_ref.shape
    own_rows, cols = w_all.shape[1:]
    ha = (cols // 128 + 1) // 2 * 128
    A, B, FULL = pl.ds(0, ha), pl.ds(ha, cols - ha), pl.ds(0, cols)
    me = lax.axis_index(axis)
    core = lax.rem(me, 2)
    chip = me // 2
    x = lax.rem(chip, 2)
    y = lax.rem(chip // 2, 2)
    z = chip // 4
    side = z // 2
    plane = [z, z + 1 - 2 * lax.rem(z, 2), 2 - side, 3 * (1 - side)]
    inner = lax.rem(z + side, 2) == 1
    outer = jnp.logical_not(inner)
    hub = core == 0
    lead = core == 1
    sends = (Keys(), Keys())
    recvs = (Keys(), Keys())

    def dev(z_, y_, x_, c_):
        return ((z_ * 2 + y_) * 2 + x_) * 2 + c_

    def xn(c_):
        return dev(z, y, 1 - x, c_)

    def yn(c_):
        return dev(z, 1 - y, x, c_)

    def peer(p, c_):
        return dev(plane[p], y, x, c_)

    partner = dev(z, y, x, 1 - core)

    def send(src, dst, role, key, to_role, recv, target, cond=None):
        c = pltpu.make_async_remote_copy(
            src_ref=src, dst_ref=dst, send_sem=send_sem.at[sends[role][key]],
            recv_sem=recv_sem.at[recv if not isinstance(recv, (str, tuple)) else recvs[to_role][recv]],
            device_id=(target,), device_id_type=MESH,
        )
        if cond is None:
            c.start()
        else:
            pl.when(cond)(c.start)

    def arrived(ref, role, key):
        pltpu.make_async_remote_copy(
            src_ref=ref, dst_ref=ref, send_sem=send_sem.at[0],
            recv_sem=recv_sem.at[recvs[role][key]],
            device_id=(partner,), device_id_type=MESH,
        ).wait_recv()

    def drained(ref, role, key):
        pltpu.make_async_remote_copy(
            src_ref=ref, dst_ref=ref, send_sem=send_sem.at[sends[role][key]],
            recv_sem=recv_sem.at[0], device_id=(partner,), device_id_type=MESH,
        ).wait_send()

    def shards(count):
        return w_all.at[pl.ds(0, count)]

    barrier = pltpu.get_barrier_semaphore()
    peers = [partner]
    for c in range(2):
        peers += [xn(c), yn(c)] + [peer(p, c) for p in range(1, 4)]
    peers += [lax.rem(me + n + s, n) for s in (-2, 2, -4, 4)]
    for p in peers:
        pl.semaphore_signal(barrier, inc=1, device_id=(p,), device_id_type=MESH)

    pairs = [
        (w_hbm, w_all.at[me]), (t_hbm, t_ref),
        (x_hbm, x_ref),
    ]
    loads = [pltpu.make_async_copy(a, b, load_sem.at[i]) for i, (a, b) in enumerate(pairs)]
    for c in loads:
        c.start()
    for c in loads[1:2]:
        c.wait()
    t = jnp.exp(jnp.full((1, 1), scalars[0], F32))
    bias = scalars[1]
    text = t_ref[...].astype(F32)
    text_length = jnp.sqrt(jnp.sum(text * text, axis=1, keepdims=True) + epsilon)
    text_low[...] = (text / text_length).astype(BF)
    loads[0].wait()

    pl.semaphore_wait(barrier, len(peers))

    part = rows // CHUNKS

    def cut_rows(c):
        return pl.ds(c * part, part)

    class Window:
        def __init__(self, key, buf, slots, mirror):
            self.key, self.buf, self.slots, self.mirror = key, buf, slots, mirror
            v = n - 1 - me if mirror else me
            q = lax.rem(v // 2, 4)
            step = 2 if mirror else -2
            back = lax.rem(me + n + step, n)
            back2 = lax.rem(me + n + 2 * step, n)
            self.back = back
            odd = lax.rem(q, 2) == 1
            even = jnp.logical_not(odd)
            self.odd, self.even, self.back2 = odd, even, back2
            self.leaf_third = 2 if mirror else 3
            self.low, self.high = slots.at[2], buf
            if not mirror:
                self.low, self.high = buf, slots.at[2]

        def at(self, slot, c):
            return self.slots.at[slot, cut_rows(c)]

        def leaf_sends(self):
            send(self.buf, self.slots.at[2], 1, (self.key, "own"), 0, (self.key, "own"), partner)

        def hub_own(self):
            send(self.buf, self.slots.at[2], 0, (self.key, "all"), 1, (self.key, "third"), partner)

        def wait_own(self):
            arrived(self.slots.at[2], 0, (self.key, "own"))

        def start_low(self, c):
            r = cut_rows(c)
            send(
                self.low.at[r], self.at(3, c), 0, (self.key, "all"), 0,
                (self.key, 3, c), self.back2,
            )
            send(
                self.low.at[r], self.at(0, c), 0, (self.key, "mixed"), 0,
                (self.key, 0, c), self.back, self.odd,
            )

        def start_high(self, c):
            r = cut_rows(c)
            send(
                self.high.at[r], self.at(1, c), 0, (self.key, "all"), 0,
                (self.key, 1, c), self.back,
            )

        def far(self, c):
            arrived(self.at(3, c), 0, (self.key, 3, c))
            send(
                self.at(3, c), self.at(0, c), 0, (self.key, "mixed"), 0,
                (self.key, 0, c), xn(0), self.even,
            )
            if not self.mirror:
                send(
                    self.at(3, c), self.at(3, c), 0, (self.key, "all"), 1,
                    (self.key, "third"), partner,
                )

        def near(self, slot, c):
            arrived(self.at(slot, c), 0, (self.key, slot, c))
            send(
                self.at(slot, c), self.at(slot, c), 0, (self.key, "all"), 1,
                (self.key, slot), partner,
            )

        def third(self):
            return 3 - core if self.mirror else 2 + core

        def leaf_wait(self, slot):
            arrived(self.slots.at[slot], 1, (self.key, slot if slot < 2 else "third"))

        def drain(self):
            @pl.when(hub)
            def _():
                drained(self.slots, 0, (self.key, "all"))
                drained(self.slots.at[0], 0, (self.key, "mixed"))

            @pl.when(lead)
            def _():
                drained(self.slots.at[0], 1, (self.key, "own"))

    def release():
        pl.semaphore_signal(credit, inc=1, device_id=(partner,), device_id_type=MESH)

    tw = Window("t", text_low, text_in, False)
    iw = Window("i", image_low, image_in, True)

    def place(r):
        return (y, 1 - y)[r in ("y", "d")], (x, 1 - x)[r in ("x", "d")]

    def pair(p, r, cut=FULL):
        y_, x_ = place(r)
        return w_all.at[pl.ds(pl.multiple_of(dev(plane[p], y_, x_, 0), 2), 2), :, cut]

    for key in ("o1", "o2", "o3", "px0", "py0"):
        recvs[1][key]
    far_key = jnp.where(inner, recvs[1]["o2"], recvs[1]["o3"])
    own = w_all.at[me]

    def wait_pair(p, r, key):
        arrived(pair(p, r), 1, key)
        send(pair(p, r), pair(p, r), 1, "w", 0, ("w", p), partner)

    def onto(p, r, cut, recv, target, key="ag", cond=None):
        send(pair(p, r, cut), pair(p, r, cut), 1, key, 1, recv, target, cond)

    def diagonal(p):
        wait_pair(p, "d", ("d", p))

    def side_x(p, key):
        arrived(pair(p, "x"), 1, key)
        onto(p, "x", A, ("d", p), yn(1))

    def side_y(p, key):
        arrived(pair(p, "y"), 1, key)
        onto(p, "y", B, ("d", p), xn(1))

    def swap(p, r):
        send(pair(p, r), pair(p, r), 1, "w", 0, ("w", p), partner)

    def first_sends(role):
        for target, recv in (
            (peer(3, 1), far_key), (peer(2, 1), far_key), (peer(1, 1), "o1"),
            (xn(1), "px0"), (yn(1), "py0"),
        ):
            send(own, own, role, "ag", 1, recv, target)

    @pl.when(hub)
    def _():
        first_sends(0)
        send(own, own, 0, "ag", 1, "w0", partner)
        tw.start_low(0)
        tw.wait_own()
        tw.start_high(0)
        for c in range(1, CHUNKS):
            pl.semaphore_wait(credit, 1)
            tw.start_low(c)
            tw.start_high(c)
        for c in range(CHUNKS):
            tw.far(c)

    @pl.when(lead)
    def _():
        first_sends(1)
        send(own, own, 1, "w", 0, ("w", 0), partner)
        tw.leaf_sends()

        side_x(0, "px0")
        onto(0, "x", FULL, ("zx", 1), peer(1, 1))
        onto(0, "x", FULL, ("zx", 2), peer(2, 1), "ag", inner)
        swap(0, "x")
        side_y(0, "py0")
        onto(0, "y", FULL, ("zy", 1), peer(1, 1))
        onto(0, "y", FULL, ("zy", 2), peer(2, 1), "ag", inner)
        swap(0, "y")
        arrived(pair(3, "o"), 1, "o3")
        onto(3, "o", FULL, "px3", xn(1))
        onto(3, "o", FULL, "py3", yn(1))
        swap(3, "o")
        arrived(pair(2, "o"), 1, "o2")
        onto(2, "o", FULL, ("zx", 2), xn(1), "ag", outer)
        onto(2, "o", FULL, ("zy", 2), yn(1), "ag", outer)
        swap(2, "o")
        wait_pair(1, "o", "o1")
        release()
        diagonal(0)
        side_x(1, ("zx", 1))
        swap(1, "x")
        side_y(1, ("zy", 1))
        swap(1, "y")
        release()
        side_x(3, "px3")
        swap(3, "x")
        side_y(3, "py3")
        swap(3, "y")
        release()
        side_x(2, ("zx", 2))
        swap(2, "x")
        side_y(2, ("zy", 2))
        swap(2, "y")
        diagonal(1)

    loads[2].wait()
    xt[...] = x_ref[...].T

    @pl.when(hub)
    def _():
        arrived(shards(7), 0, ("w", 0))
        arrived(shards(8), 0, ("w", 1))

    def project(p):
        at = pl.ds(pl.multiple_of(plane[p] * 8 * own_rows, 8 * own_rows), 8 * own_rows)
        rows_of = w_all[pl.ds(pl.multiple_of(plane[p] * 8, 8), 8)].reshape(8 * own_rows, cols)
        return jnp.dot(x_ref[:, at], rows_of, preferred_element_type=F32)

    @pl.when(lead)
    def _():
        arrived(w_all.at[partner], 1, "w0")

    embedded_ref[...] = project(0)
    embedded_ref[...] += project(1)

    @pl.when(hub)
    def _():
        for c in range(CHUNKS):
            tw.near(1, c)
        arrived(shards(8), 0, ("w", 3))

    @pl.when(lead)
    def _():
        diagonal(3)

    embedded_ref[...] += project(3)

    @pl.when(hub)
    def _():
        for c in range(CHUNKS):
            tw.near(0, c)
        arrived(shards(8), 0, ("w", 2))

    @pl.when(lead)
    def _():
        diagonal(2)

    weight = w_all[...].reshape(n * own_rows, cols)
    embedded = embedded_ref[...] + project(2)
    image_length = jnp.sqrt(jnp.sum(embedded * embedded, axis=1, keepdims=True) + epsilon)
    image_unit = embedded / image_length
    image_low[...] = image_unit.astype(BF)

    @pl.when(hub)
    def _():
        iw.hub_own()
        for c in range(3):
            iw.start_high(c)

    @pl.when(lead)
    def _():
        iw.leaf_sends()

    mine = image_low[...]
    own_text = text_low[...]
    grad = pair_grad(mine, own_text, t, bias, True)
    image_grad = jnp.dot(grad, own_text, preferred_element_type=F32)

    @pl.when(hub)
    def _():
        iw.wait_own()
        for c in range(3):
            iw.start_low(c)

    def window(low, win, grads):
        for i, q in enumerate((win.third(), 1, 0)):
            @pl.when(lead)
            def _():
                win.leaf_wait((win.leaf_third, 1, 0)[i])

            block = win.slots[q]
            grads += jnp.dot(
                pair_grad(low, block, t, bias, False), block, preferred_element_type=F32
            )
        return grads

    image_grad = window(mine, tw, image_grad)
    along = jnp.sum(image_unit * image_grad, axis=1, keepdims=True)
    embed_grad = ((image_grad - image_unit * along) / image_length).astype(BF)

    def hand_over(p, r):
        y_, x_ = place(r)
        c = y_ * 2 + x_
        key = ("g0", p, "d" if r == "d" else "rest")
        send(to_core.at[p, c], from_core.at[p, c], 0, "g0", 1, key, partner)

    group = 8 * own_rows
    for p in (3, 2, 1, 0):
        lhs = xt[pl.ds(pl.multiple_of(plane[p] * group, group), group), :]
        product = jnp.dot(lhs, embed_grad, preferred_element_type=F32)
        gz[p] = product.reshape(4, 2, own_rows, cols)

        @pl.when(hub)
        def _():
            to_core[p] = gz[p].astype(BF)
            hand_over(p, "d")

    @pl.when(hub)
    def _():
        for p in (3, 2, 1, 0):
            for r in ("x", "y", "o"):
                hand_over(p, r)

    S_O, S_X, S_Y, S_D = range(4)

    def base(p, r, cut):
        y_, x_ = place(r)
        c = y_ * 2 + x_
        return gz[p, c, :, :, cut] + from_core[p, c, :, :, cut].astype(F32)

    def put(p, r, cut, value):
        out_s[p, r, :, :, cut] = value.astype(BF)

    def open_plane(p):
        arrived(from_core.at[p, 0], 1, ("g0", p, "d"))
        put(p, S_D, FULL, base(p, "d", FULL))
        send(out_s.at[p, S_D, :, :, A], in_d.at[p, :, :, A], 1, "rs", 1, ("gd", p), yn(1))
        send(out_s.at[p, S_D, :, :, B], in_d.at[p, :, :, B], 1, "rs", 1, ("gd", p), xn(1))

    for key in ("g1o", "g2o", "g3o"):
        recvs[1][key]
    gs_key = jnp.where(inner, recvs[1]["g2o"], recvs[1]["g3o"])
    gs_slot = jnp.where(inner, 1, 2)

    def rest(p):
        arrived(from_core.at[p, pl.ds(0, 3)], 1, ("g0", p, "rest"))

    def sides(p):
        arrived(in_d.at[p], 1, ("gd", p))

    def x_sum(p, cut):
        v = base(p, "x", cut)
        return v + in_d[p, :, :, cut].astype(F32) if cut is A else v

    def y_sum(p, cut):
        v = base(p, "y", cut)
        return v + in_d[p, :, :, cut].astype(F32) if cut is B else v

    def fill_sides(p):
        sides(p)
        for cut in (A, B):
            put(p, S_X, cut, x_sum(p, cut))
            put(p, S_Y, cut, y_sum(p, cut))

    @pl.when(lead)
    def _():
        open_plane(3)
        open_plane(2)
        open_plane(1)
        rest(3)
        rest(2)

        @pl.when(inner)
        def _():
            put(2, S_O, FULL, base(2, "o", FULL))
            send(out_s.at[2, S_O], in_z.at[gs_slot, 0], 1, "rs", 1, gs_key, peer(2, 1))

        rest(1)
        put(1, S_O, FULL, base(1, "o", FULL))
        send(out_s.at[1, S_O], in_z.at[0, 0], 1, "rs", 1, "g1o", peer(1, 1))
        fill_sides(3)
        send(out_s.at[3, S_X], in_xy.at[0], 1, "rs", 1, "gxy3", xn(1))
        send(out_s.at[3, S_Y], in_xy.at[1], 1, "rs", 1, "gxy3", yn(1))
        release()
        open_plane(0)
        rest(0)

    @pl.when(hub)
    def _():
        for c in range(3):
            iw.far(c)
        for c in range(3, CHUNKS):
            pl.semaphore_wait(credit, 1)
            iw.start_low(c)
            iw.start_high(c)
        for c in range(3, CHUNKS):
            iw.far(c)
        for c in range(CHUNKS):
            iw.near(1, c)
        for c in range(CHUNKS):
            iw.near(0, c)

    @pl.when(lead)
    def _():
        fill_sides(2)

        @pl.when(outer)
        def _():
            send(out_s.at[2, S_X], in_e.at[0], 1, "rs", 1, "ge", xn(1))
            send(out_s.at[2, S_Y], in_e.at[1], 1, "rs", 1, "ge", yn(1))

        @pl.when(inner)
        def _():
            send(out_s.at[2, S_X], in_z.at[1, 1], 1, "rs", 1, "g2xy", peer(2, 1))
            send(out_s.at[2, S_Y], in_z.at[1, 2], 1, "rs", 1, "g2xy", peer(2, 1))

        fill_sides(1)
        send(out_s.at[1, S_X], in_z.at[0, 1], 1, "rs", 1, "g1xy", peer(1, 1))
        send(out_s.at[1, S_Y], in_z.at[0, 2], 1, "rs", 1, "g1xy", peer(1, 1))

    gx_ref[...] = dot_nt(embed_grad, weight).astype(BF)

    @pl.when(lead)
    def _():
        arrived(in_xy, 1, "gxy3")
        put(
            3, S_O, FULL,
            base(3, "o", FULL) + in_xy[0].astype(F32) + in_xy[1].astype(F32),
        )
        send(out_s.at[3, S_O], in_z.at[gs_slot, 0], 1, "rs", 1, gs_key, peer(3, 1))

        @pl.when(outer)
        def _():
            arrived(in_e, 1, "ge")
            put(
                2, S_O, FULL,
                base(2, "o", FULL) + in_e[0].astype(F32) + in_e[1].astype(F32),
            )
            send(out_s.at[2, S_O], in_z.at[gs_slot, 0], 1, "rs", 1, gs_key, peer(2, 1))


    text_grad = jnp.dot(
        pair_grad(own_text, mine, t, bias, True), mine, preferred_element_type=F32
    )

    @pl.when(lead)
    def _():
        sides(0)
        arrived(in_z.at[0, pl.ds(1, 2)], 1, "g1xy")


        @pl.when(outer)
        def _():
            for cut in (A, B):
                put(0, S_X, cut, x_sum(0, cut) + in_z[0, 1, :, :, cut].astype(F32))
                put(0, S_Y, cut, y_sum(0, cut) + in_z[0, 2, :, :, cut].astype(F32))

        @pl.when(inner)
        def _():
            arrived(in_z.at[1, pl.ds(1, 2)], 1, "g2xy")
            for cut in (A, B):
                for r, fill in ((1, x_sum), (2, y_sum)):
                    put(
                        0, r, cut,
                        fill(0, cut) + in_z[0, r, :, :, cut].astype(F32)
                        + in_z[1, r, :, :, cut].astype(F32),
                    )

        for c in range(2):
            send(out_s.at[0, S_X, c], in_fin.at[0], 1, "rs", c, "fin", xn(c))
            send(out_s.at[0, S_Y, c], in_fin.at[1], 1, "rs", c, "fin", yn(c))

    text_grad = window(own_text, iw, text_grad)
    text_unit = t_ref[...].astype(F32) / text_length
    along = jnp.sum(text_unit * text_grad, axis=1, keepdims=True)
    gt_ref[...] = ((text_grad - text_unit * along) / text_length).astype(BF)

    @pl.when(lead)
    def _():
        total = base(0, "o", FULL)
        for i, key in enumerate(("g1o", "g2o", "g3o")):
            arrived(in_z.at[i, 0], 1, key)
            total += in_z[i, 0].astype(F32)
        pre_out[...] = total[0]
        send(pre_out, pre_in, 1, "pre", 0, "pre", partner)
        pre_in[...] = total[1]
        arrived(in_fin, 1, "fin")

    @pl.when(hub)
    def _():
        arrived(pre_in, 0, "pre")
        arrived(in_fin, 0, "fin")

    gw_ref[...] = pre_in[...] + in_fin[0].astype(F32) + in_fin[1].astype(F32)

    tw.drain()
    iw.drain()

    @pl.when(hub)
    def _():
        drained(shards(6), 0, "ag")
        drained(shards(n), 0, "g0")

    @pl.when(lead)
    def _():
        drained(shards(25), 1, "ag")
        drained(shards(n - 1), 1, "w")
        drained(shards(30), 1, "rs")
        drained(pre_out, 1, "pre")

    assert max(map(len, sends)) <= SENDS
    assert max(map(len, recvs)) <= RECVS


def fused(n, axis, image_features, head_weight, text_embeds, factor, bias):
    rows, width = image_features.shape
    own_rows, cols = head_weight.shape
    hbm = pl.BlockSpec(memory_space=pltpu.HBM)
    vmem = pl.BlockSpec(memory_space=pltpu.VMEM)
    two = (2, own_rows, cols)
    scratch = [
        ((rows, width), BF),
        ((rows, cols), BF),
        ((n, own_rows, cols), BF),
        ((rows, cols), BF),
        ((5, rows, cols), BF),
        ((rows, cols), BF),
        ((5, rows, cols), BF),
        ((width, rows), BF),
        ((4, 4) + two, F32),
        ((4, 4) + two, BF),
        ((4, 4) + two, BF),
        ((4, 4) + two, BF),
        ((4,) + two, BF),
        ((2,) + two, BF),
        ((3, 3) + two, BF),
        ((2,) + two, BF),
        (two, BF),
        ((own_rows, cols), F32),
        ((own_rows, cols), F32),
        ((rows, cols), F32),
    ]
    shapes = (((rows, width), BF), ((rows, cols), BF), ((own_rows, cols), F32))
    results = pl.pallas_call(
        functools.partial(kernel, n, axis),
        out_shape=tuple(pltpu.VMEM(s, d) for s, d in shapes),
        in_specs=[hbm] * 3 + [pl.BlockSpec(memory_space=pltpu.SMEM)],
        out_specs=(vmem, vmem, vmem),
        scratch_shapes=[pltpu.VMEM(s, d) for s, d in scratch]
        + [pltpu.SemaphoreType.DMA((k,)) for k in (5, SENDS, RECVS)]
        + [pltpu.SemaphoreType.REGULAR],
        compiler_params=pltpu.CompilerParams(
            collective_id=0, has_side_effects=True, vmem_limit_bytes=65413120
        ),
    )(image_features, head_weight, text_embeds, jnp.concatenate([factor, bias]))
    return pl.pallas_call(
        write_out,
        out_shape=tuple(jax.ShapeDtypeStruct(s, d) for s, d in shapes),
        in_specs=[vmem] * 3,
        out_specs=(hbm,) * 3,
        scratch_shapes=[pltpu.SemaphoreType.DMA((3,))],
        compiler_params=pltpu.CompilerParams(vmem_limit_bytes=2**20),
    )(*results)


def write_out(gx, gt, gw, gx_out, gt_out, gw_out, sems):
    pairs = ((gx, gx_out), (gt, gt_out), (gw, gw_out))
    copies = [pltpu.make_async_copy(a, b, sems.at[i]) for i, (a, b) in enumerate(pairs)]
    for c in copies:
        c.start()
    for c in copies:
        c.wait()


def passed_along(block, axis, distance):
    devices = range(lax.axis_size(axis))
    route = [((i - distance) % len(devices), i) for i in devices]
    return lax.ppermute(block, axis, route)


def normalize(rows):
    squares = jnp.sum(rows * rows, axis=1, keepdims=True)
    length = jnp.sqrt(squares + epsilon)
    return (rows / length, length)


def similarity_derivative(
    picture_sample_group,
    caption_sample_group,
    similarity_multiplier,
    neighbour_distance,
    outer_dimension_size,
):
    similarity_matrix = (
        similarity_multiplier
        * lax.dot_general(
            picture_sample_group,
            caption_sample_group,
            (((1,), (1,)), ((), ())),
            preferred_element_type=jnp.float32,
        )
        + neighbour_distance
    )
    if outer_dimension_size:
        matched = lax.broadcasted_iota(
            jnp.int32, similarity_matrix.shape, 0
        ) == lax.broadcasted_iota(jnp.int32, similarity_matrix.shape, 1)
        match_polarity = jnp.where(matched, 1.0, -1.0).astype(jnp.float32)
    else:
        match_polarity = -jnp.ones(similarity_matrix.shape, jnp.float32)
    return (
        -similarity_multiplier
        * match_polarity
        * jax.nn.sigmoid(-match_polarity * similarity_matrix)
    ).astype(jnp.bfloat16)


def project_back(grad, unit_rows, length):
    return (grad - unit_rows * jnp.sum(unit_rows * grad, axis=1, keepdims=True)) / length


def by_collectives(image_features, head_weight, text_embeds, natural_exponent_factor, logit_bias):
    full_weight = lax.all_gather(head_weight, "blk", axis=0, tiled=True)
    embedded = jnp.dot(image_features, full_weight, preferred_element_type=jnp.float32)
    image_unit, image_length = normalize(embedded)
    picture_embedding_mapped = image_unit.astype(jnp.bfloat16)
    text_unit, text_length = normalize(text_embeds.astype(jnp.float32))
    text_low = text_unit.astype(jnp.bfloat16)
    similarity_multiplier = jnp.exp(natural_exponent_factor[0])
    neighbour_distance = logit_bias[0]
    image_grad = jnp.zeros(image_unit.shape, jnp.float32)
    current_neighbour_tile = text_low
    for partition_portion in range(S):
        mapping_matrix = similarity_derivative(
            picture_embedding_mapped,
            current_neighbour_tile,
            similarity_multiplier,
            neighbour_distance,
            partition_portion == 0,
        )
        image_grad = image_grad + jnp.dot(
            mapping_matrix, current_neighbour_tile, preferred_element_type=jnp.float32
        )
        if partition_portion + 1 < S:
            current_neighbour_tile = passed_along(current_neighbour_tile, "blk", -1)
    text_grad = jnp.zeros(text_unit.shape, jnp.float32)
    passing = picture_embedding_mapped
    for partition_portion in range(S):
        mapping_matrix = similarity_derivative(
            passing, text_low, similarity_multiplier, neighbour_distance, partition_portion == 0
        )
        text_grad = text_grad + lax.dot_general(
            mapping_matrix, passing, (((0,), (0,)), ((), ())), preferred_element_type=jnp.float32
        )
        if partition_portion + 1 < S:
            passing = passed_along(passing, "blk", 1)
    embed_grad = project_back(image_grad, image_unit, image_length).astype(jnp.bfloat16)
    grad_text = project_back(text_grad, text_unit, text_length).astype(jnp.bfloat16)
    grad_features = lax.dot_general(
        embed_grad, full_weight, (((1,), (1,)), ((), ())), preferred_element_type=jnp.float32
    ).astype(jnp.bfloat16)
    grad_weight = lax.psum_scatter(
        lax.dot_general(
            image_features, embed_grad, (((0,), (0,)), ((), ())), preferred_element_type=jnp.float32
        ),
        "blk",
        scatter_dimension=0,
        tiled=True,
    )
    return (grad_features, grad_text, grad_weight)


def on_device(image_features, head_weight, text_embeds, natural_exponent_factor, logit_bias):
    n = lax.axis_size("blk")
    whole_tiles = head_weight.shape[0] % 16 == 0 and n % 8 == 0 and n // 8 == 4
    run = functools.partial(fused, n, "blk") if whole_tiles else by_collectives
    return run(image_features, head_weight, text_embeds, natural_exponent_factor, logit_bias)


def solution(mesh):
    return jax.shard_map(
        on_device,
        mesh=mesh,
        in_specs=(P("blk", None), P("blk", None), P("blk", None), P(), P()),
        out_specs=(P("blk", None), P("blk", None), P("blk", None)),
        check_vma=False,
    )
```

```python
import functools

import jax
import jax.numpy as jnp
from jax import lax
from jax.experimental import pallas as pl
from jax.experimental.pallas import tpu as pltpu
from jax.sharding import PartitionSpec as P

S = 4
epsilon = 1e-06
MESH = pl.DeviceIdType.MESH
F32 = jnp.float32
BF = jnp.bfloat16


def dot_nt(a, b):
    return lax.dot_general(a, b, (((1,), (1,)), ((), ())), preferred_element_type=F32)


def pair_grad(rows, cols, t, bias, own):
    logits = t * dot_nt(rows, cols) + bias
    if own:
        matched = lax.broadcasted_iota(jnp.int32, logits.shape, 0) == lax.broadcasted_iota(
            jnp.int32, logits.shape, 1
        )
        z = jnp.where(matched, 1.0, -1.0).astype(F32)
        return (-t * z * jax.nn.sigmoid(-z * logits)).astype(BF)
    return (t * jax.nn.sigmoid(logits)).astype(BF)


CHUNKS = 4
SENDS = 16
RECVS = 48


class Keys(dict):
    def __missing__(self, key):
        self[key] = len(self)
        return self[key]


def kernel(
    n, axis,
    x_hbm, w_hbm, t_hbm, lf_hbm, bias_hbm,
    gx_ref, gt_ref, gw_ref,
    x_ref, t_ref, w_all, text_low, text_in, image_low, image_in, xt, gz, from_core, to_core,
    out_s, in_d, in_xy, in_z, in_e, in_fin, pre_out, pre_in, embedded_ref,
    factor_ref, bias_ref, load_sem, send_sem, recv_sem, credit,
):
    rows, width = x_ref.shape
    own_rows, cols = w_all.shape[1:]
    ha = (cols // 128 + 1) // 2 * 128
    A, B, FULL = pl.ds(0, ha), pl.ds(ha, cols - ha), pl.ds(0, cols)
    me = lax.axis_index(axis)
    core = lax.rem(me, 2)
    chip = me // 2
    x = lax.rem(chip, 2)
    y = lax.rem(chip // 2, 2)
    z = chip // 4
    side = z // 2
    plane = [z, z + 1 - 2 * lax.rem(z, 2), 2 - side, 3 * (1 - side)]
    inner = lax.rem(z + side, 2) == 1
    outer = jnp.logical_not(inner)
    hub = core == 0
    lead = core == 1
    sends = (Keys(), Keys())
    recvs = (Keys(), Keys())

    def dev(z_, y_, x_, c_):
        return ((z_ * 2 + y_) * 2 + x_) * 2 + c_

    def xn(c_):
        return dev(z, y, 1 - x, c_)

    def yn(c_):
        return dev(z, 1 - y, x, c_)

    def peer(p, c_):
        return dev(plane[p], y, x, c_)

    partner = dev(z, y, x, 1 - core)

    def send(src, dst, role, key, to_role, recv, target, cond=None):
        c = pltpu.make_async_remote_copy(
            src_ref=src, dst_ref=dst, send_sem=send_sem.at[sends[role][key]],
            recv_sem=recv_sem.at[recv if not isinstance(recv, (str, tuple)) else recvs[to_role][recv]],
            device_id=(target,), device_id_type=MESH,
        )
        if cond is None:
            c.start()
        else:
            pl.when(cond)(c.start)

    def arrived(ref, role, key):
        pltpu.make_async_remote_copy(
            src_ref=ref, dst_ref=ref, send_sem=send_sem.at[0],
            recv_sem=recv_sem.at[recvs[role][key]],
            device_id=(partner,), device_id_type=MESH,
        ).wait_recv()

    def drained(ref, role, key):
        pltpu.make_async_remote_copy(
            src_ref=ref, dst_ref=ref, send_sem=send_sem.at[sends[role][key]],
            recv_sem=recv_sem.at[0], device_id=(partner,), device_id_type=MESH,
        ).wait_send()

    def shards(count):
        return w_all.at[pl.ds(0, count)]

    barrier = pltpu.get_barrier_semaphore()
    peers = [partner]
    for c in range(2):
        peers += [xn(c), yn(c)] + [peer(p, c) for p in range(1, 4)]
    peers += [lax.rem(me + n + s, n) for s in (-2, 2, -4, 4)]
    for p in peers:
        pl.semaphore_signal(barrier, inc=1, device_id=(p,), device_id_type=MESH)

    pairs = [
        (w_hbm, w_all.at[me]), (t_hbm, t_ref), (lf_hbm, factor_ref), (bias_hbm, bias_ref),
        (x_hbm, x_ref),
    ]
    loads = [pltpu.make_async_copy(a, b, load_sem.at[i]) for i, (a, b) in enumerate(pairs)]
    for c in loads:
        c.start()
    loads[0].wait()

    pl.semaphore_wait(barrier, len(peers))

    part = rows // CHUNKS

    def cut_rows(c):
        return pl.ds(c * part, part)

    class Window:
        def __init__(self, key, buf, slots, mirror):
            self.key, self.buf, self.slots, self.mirror = key, buf, slots, mirror
            v = n - 1 - me if mirror else me
            q = lax.rem(v // 2, 4)
            step = 2 if mirror else -2
            back = lax.rem(me + n + step, n)
            back2 = lax.rem(me + n + 2 * step, n)
            self.back = back
            odd = lax.rem(q, 2) == 1
            even = jnp.logical_not(odd)
            self.odd, self.even, self.back2 = odd, even, back2
            self.leaf_third = 2 if mirror else 3
            self.low, self.high = slots.at[2], buf
            if not mirror:
                self.low, self.high = buf, slots.at[2]

        def at(self, slot, c):
            return self.slots.at[slot, cut_rows(c)]

        def leaf_sends(self):
            send(self.buf, self.slots.at[2], 1, (self.key, "own"), 0, (self.key, "own"), partner)

        def hub_own(self):
            send(self.buf, self.slots.at[2], 0, (self.key, "all"), 1, (self.key, "third"), partner)

        def wait_own(self):
            arrived(self.slots.at[2], 0, (self.key, "own"))

        def start_low(self, c):
            r = cut_rows(c)
            send(
                self.low.at[r], self.at(3, c), 0, (self.key, "all"), 0,
                (self.key, 3, c), self.back2,
            )
            send(
                self.low.at[r], self.at(0, c), 0, (self.key, "mixed"), 0,
                (self.key, 0, c), self.back, self.odd,
            )

        def start_high(self, c):
            r = cut_rows(c)
            send(
                self.high.at[r], self.at(1, c), 0, (self.key, "all"), 0,
                (self.key, 1, c), self.back,
            )

        def far(self, c):
            arrived(self.at(3, c), 0, (self.key, 3, c))
            send(
                self.at(3, c), self.at(0, c), 0, (self.key, "mixed"), 0,
                (self.key, 0, c), xn(0), self.even,
            )
            if not self.mirror:
                send(
                    self.at(3, c), self.at(3, c), 0, (self.key, "all"), 1,
                    (self.key, "third"), partner,
                )

        def near(self, slot, c):
            arrived(self.at(slot, c), 0, (self.key, slot, c))
            send(
                self.at(slot, c), self.at(slot, c), 0, (self.key, "all"), 1,
                (self.key, slot), partner,
            )

        def third(self):
            return 3 - core if self.mirror else 2 + core

        def leaf_wait(self, slot):
            arrived(self.slots.at[slot], 1, (self.key, slot if slot < 2 else "third"))

        def drain(self):
            @pl.when(hub)
            def _():
                drained(self.slots, 0, (self.key, "all"))
                drained(self.slots.at[0], 0, (self.key, "mixed"))

            @pl.when(lead)
            def _():
                drained(self.slots.at[0], 1, (self.key, "own"))

    def release():
        pl.semaphore_signal(credit, inc=1, device_id=(partner,), device_id_type=MESH)

    tw = Window("t", text_low, text_in, False)
    iw = Window("i", image_low, image_in, True)

    def place(r):
        return (y, 1 - y)[r in ("y", "d")], (x, 1 - x)[r in ("x", "d")]

    def pair(p, r, cut=FULL):
        y_, x_ = place(r)
        return w_all.at[pl.ds(pl.multiple_of(dev(plane[p], y_, x_, 0), 2), 2), :, cut]

    for key in ("o1", "o2", "o3", "px0", "py0"):
        recvs[1][key]
    far_key = jnp.where(inner, recvs[1]["o2"], recvs[1]["o3"])
    own = w_all.at[me]

    def wait_pair(p, r, key):
        arrived(pair(p, r), 1, key)
        send(pair(p, r), pair(p, r), 1, "w", 0, ("w", p), partner)

    def onto(p, r, cut, recv, target, key="ag", cond=None):
        send(pair(p, r, cut), pair(p, r, cut), 1, key, 1, recv, target, cond)

    def diagonal(p):
        wait_pair(p, "d", ("d", p))

    def side_x(p, key):
        arrived(pair(p, "x"), 1, key)
        onto(p, "x", A, ("d", p), yn(1))

    def side_y(p, key):
        arrived(pair(p, "y"), 1, key)
        onto(p, "y", B, ("d", p), xn(1))

    def swap(p, r):
        send(pair(p, r), pair(p, r), 1, "w", 0, ("w", p), partner)

    def first_sends(role):
        for target, recv in (
            (peer(3, 1), far_key), (peer(2, 1), far_key), (peer(1, 1), "o1"),
            (xn(1), "px0"), (yn(1), "py0"),
        ):
            send(own, own, role, "ag", 1, recv, target)

    @pl.when(hub)
    def _():
        first_sends(0)
        send(own, own, 0, "ag", 1, "w0", partner)

    @pl.when(lead)
    def _():
        first_sends(1)
        send(own, own, 1, "w", 0, ("w", 0), partner)

    for c in loads[1:4]:
        c.wait()
    t = jnp.exp(jnp.full((1, 1), factor_ref[0], F32))
    bias = bias_ref[0]
    text = t_ref[...].astype(F32)
    text_length = jnp.sqrt(jnp.sum(text * text, axis=1, keepdims=True) + epsilon)
    text_low[...] = (text / text_length).astype(BF)

    @pl.when(hub)
    def _():
        tw.start_low(0)
        tw.wait_own()
        tw.start_high(0)
        for c in range(1, CHUNKS):
            pl.semaphore_wait(credit, 1)
            tw.start_low(c)
            tw.start_high(c)
            tw.far(c - 1)
        tw.far(CHUNKS - 1)

    @pl.when(lead)
    def _():
        tw.leaf_sends()

        side_x(0, "px0")
        onto(0, "x", FULL, ("zx", 1), peer(1, 1))
        onto(0, "x", FULL, ("zx", 2), peer(2, 1), "ag", inner)
        swap(0, "x")
        side_y(0, "py0")
        onto(0, "y", FULL, ("zy", 1), peer(1, 1))
        onto(0, "y", FULL, ("zy", 2), peer(2, 1), "ag", inner)
        swap(0, "y")
        arrived(pair(3, "o"), 1, "o3")
        onto(3, "o", FULL, "px3", xn(1))
        onto(3, "o", FULL, "py3", yn(1))
        swap(3, "o")
        arrived(pair(2, "o"), 1, "o2")
        onto(2, "o", FULL, ("zx", 2), xn(1), "ag", outer)
        onto(2, "o", FULL, ("zy", 2), yn(1), "ag", outer)
        swap(2, "o")
        wait_pair(1, "o", "o1")
        release()
        diagonal(0)
        side_x(1, ("zx", 1))
        swap(1, "x")
        side_y(1, ("zy", 1))
        swap(1, "y")
        release()
        side_x(3, "px3")
        swap(3, "x")
        side_y(3, "py3")
        swap(3, "y")
        release()
        side_x(2, ("zx", 2))
        swap(2, "x")
        side_y(2, ("zy", 2))
        swap(2, "y")
        diagonal(1)

    loads[4].wait()
    xt[...] = x_ref[...].T

    @pl.when(hub)
    def _():
        arrived(shards(7), 0, ("w", 0))
        arrived(shards(8), 0, ("w", 1))

    def project(p):
        at = pl.ds(pl.multiple_of(plane[p] * 8 * own_rows, 8 * own_rows), 8 * own_rows)
        rows_of = w_all[pl.ds(pl.multiple_of(plane[p] * 8, 8), 8)].reshape(8 * own_rows, cols)
        return jnp.dot(x_ref[:, at], rows_of, preferred_element_type=F32)

    @pl.when(lead)
    def _():
        arrived(w_all.at[partner], 1, "w0")

    embedded_ref[...] = project(0)
    embedded_ref[...] += project(1)

    @pl.when(hub)
    def _():
        for c in range(CHUNKS):
            tw.near(1, c)
        arrived(shards(8), 0, ("w", 3))

    @pl.when(lead)
    def _():
        diagonal(3)

    embedded_ref[...] += project(3)

    @pl.when(hub)
    def _():
        for c in range(CHUNKS):
            tw.near(0, c)
        arrived(shards(8), 0, ("w", 2))

    @pl.when(lead)
    def _():
        diagonal(2)

    weight = w_all[...].reshape(n * own_rows, cols)
    embedded = embedded_ref[...] + project(2)
    image_length = jnp.sqrt(jnp.sum(embedded * embedded, axis=1, keepdims=True) + epsilon)
    image_unit = embedded / image_length
    image_low[...] = image_unit.astype(BF)

    @pl.when(hub)
    def _():
        iw.hub_own()
        for c in range(3):
            iw.start_high(c)

    @pl.when(lead)
    def _():
        iw.leaf_sends()

    mine = image_low[...]
    own_text = text_low[...]
    grad = pair_grad(mine, own_text, t, bias, True)
    image_grad = jnp.dot(grad, own_text, preferred_element_type=F32)

    @pl.when(hub)
    def _():
        iw.wait_own()
        for c in range(3):
            iw.start_low(c)

    def window(low, win, grads):
        for i, q in enumerate((win.third(), 1, 0)):
            @pl.when(lead)
            def _():
                win.leaf_wait((win.leaf_third, 1, 0)[i])

            block = win.slots[q]
            grads += jnp.dot(
                pair_grad(low, block, t, bias, False), block, preferred_element_type=F32
            )
        return grads

    image_grad = window(mine, tw, image_grad)
    along = jnp.sum(image_unit * image_grad, axis=1, keepdims=True)
    embed_grad = ((image_grad - image_unit * along) / image_length).astype(BF)

    def hand_over(p, r):
        y_, x_ = place(r)
        c = y_ * 2 + x_
        key = ("g0", p, "d" if r == "d" else "rest")
        send(to_core.at[p, c], from_core.at[p, c], 0, "g0", 1, key, partner)

    group = 8 * own_rows
    for p in (3, 2, 1, 0):
        lhs = xt[pl.ds(pl.multiple_of(plane[p] * group, group), group), :]
        product = jnp.dot(lhs, embed_grad, preferred_element_type=F32)
        gz[p] = product.reshape(4, 2, own_rows, cols)

        @pl.when(hub)
        def _():
            to_core[p] = gz[p].astype(BF)
            hand_over(p, "d")

    @pl.when(hub)
    def _():
        for p in (3, 2, 1, 0):
            for r in ("x", "y", "o"):
                hand_over(p, r)

    S_O, S_X, S_Y, S_D = range(4)

    def base(p, r, cut):
        y_, x_ = place(r)
        c = y_ * 2 + x_
        return gz[p, c, :, :, cut] + from_core[p, c, :, :, cut].astype(F32)

    def put(p, r, cut, value):
        out_s[p, r, :, :, cut] = value.astype(BF)

    def open_plane(p):
        arrived(from_core.at[p, 0], 1, ("g0", p, "d"))
        put(p, S_D, FULL, base(p, "d", FULL))
        send(out_s.at[p, S_D, :, :, A], in_d.at[p, :, :, A], 1, "rs", 1, ("gd", p), yn(1))
        send(out_s.at[p, S_D, :, :, B], in_d.at[p, :, :, B], 1, "rs", 1, ("gd", p), xn(1))

    for key in ("g1o", "g2o", "g3o"):
        recvs[1][key]
    gs_key = jnp.where(inner, recvs[1]["g2o"], recvs[1]["g3o"])
    gs_slot = jnp.where(inner, 1, 2)

    def rest(p):
        arrived(from_core.at[p, pl.ds(0, 3)], 1, ("g0", p, "rest"))

    def sides(p):
        arrived(in_d.at[p], 1, ("gd", p))

    def x_sum(p, cut):
        v = base(p, "x", cut)
        return v + in_d[p, :, :, cut].astype(F32) if cut is A else v

    def y_sum(p, cut):
        v = base(p, "y", cut)
        return v + in_d[p, :, :, cut].astype(F32) if cut is B else v

    def put_sides(p, first):
        cx, cy = (B, A) if first else (A, B)
        put(p, S_X, cx, x_sum(p, cx))
        put(p, S_Y, cy, y_sum(p, cy))

    def send_sides(p, first, buf, i, key, tx, ty):
        cx, cy = (B, A) if first else (A, B)
        for r, cut, target in ((0, cx, tx), (1, cy, ty)):
            dst = buf.at[r, :, :, cut] if i is None else buf.at[i, r + 1, :, :, cut]
            send(out_s.at[p, S_X + r, :, :, cut], dst, 1, "rs", 1, key, target)

    def sides_of(p, first):
        if not first:
            sides(p)
        put_sides(p, first)
        if p == 3:
            send_sides(p, first, in_xy, None, "gxy3", xn(1), yn(1))
        if p == 1:
            send_sides(p, first, in_z, 0, "g1xy", peer(1, 1), peer(1, 1))
        if p == 2:
            @pl.when(outer)
            def _():
                send_sides(p, first, in_e, None, "ge", xn(1), yn(1))

            @pl.when(inner)
            def _():
                send_sides(p, first, in_z, 1, "g2xy", peer(2, 1), peer(2, 1))

    gx_ref[...] = dot_nt(embed_grad, weight).astype(BF)

    text_grad = jnp.dot(
        pair_grad(own_text, mine, t, bias, True), mine, preferred_element_type=F32
    )

    @pl.when(lead)
    def _():
        open_plane(3)
        open_plane(2)
        open_plane(1)
        rest(3)
        sides_of(3, True)
        rest(2)

        @pl.when(inner)
        def _():
            put(2, S_O, FULL, base(2, "o", FULL))
            send(out_s.at[2, S_O], in_z.at[gs_slot, 0], 1, "rs", 1, gs_key, peer(2, 1))

        sides_of(2, True)
        rest(1)
        put(1, S_O, FULL, base(1, "o", FULL))
        send(out_s.at[1, S_O], in_z.at[0, 0], 1, "rs", 1, "g1o", peer(1, 1))
        sides_of(1, True)
        sides_of(3, False)
        release()
        open_plane(0)
        rest(0)

    @pl.when(hub)
    def _():
        for c in range(3):
            iw.far(c)
        for c in range(3, CHUNKS):
            pl.semaphore_wait(credit, 1)
            iw.start_low(c)
            iw.start_high(c)
        for c in range(3, CHUNKS):
            iw.far(c)
        for c in range(CHUNKS):
            iw.near(1, c)
        for c in range(CHUNKS):
            iw.near(0, c)

    @pl.when(lead)
    def _():
        sides_of(2, False)
        sides_of(1, False)

    @pl.when(lead)
    def _():
        arrived(in_xy, 1, "gxy3")
        put(
            3, S_O, FULL,
            base(3, "o", FULL) + in_xy[0].astype(F32) + in_xy[1].astype(F32),
        )
        send(out_s.at[3, S_O], in_z.at[gs_slot, 0], 1, "rs", 1, gs_key, peer(3, 1))

    @pl.when(lead)
    def _():
        sides(0)
        arrived(in_z.at[0, pl.ds(1, 2)], 1, "g1xy")


        @pl.when(outer)
        def _():
            for cut in (A, B):
                put(0, S_X, cut, x_sum(0, cut) + in_z[0, 1, :, :, cut].astype(F32))
                put(0, S_Y, cut, y_sum(0, cut) + in_z[0, 2, :, :, cut].astype(F32))

        @pl.when(inner)
        def _():
            arrived(in_z.at[1, pl.ds(1, 2)], 1, "g2xy")
            for cut in (A, B):
                for r, fill in ((1, x_sum), (2, y_sum)):
                    put(
                        0, r, cut,
                        fill(0, cut) + in_z[0, r, :, :, cut].astype(F32)
                        + in_z[1, r, :, :, cut].astype(F32),
                    )

        for c in range(2):
            send(out_s.at[0, S_X, c], in_fin.at[0], 1, "rs", c, "fin", xn(c))
            send(out_s.at[0, S_Y, c], in_fin.at[1], 1, "rs", c, "fin", yn(c))

        @pl.when(outer)
        def _():
            arrived(in_e, 1, "ge")
            put(
                2, S_O, FULL,
                base(2, "o", FULL) + in_e[0].astype(F32) + in_e[1].astype(F32),
            )
            send(out_s.at[2, S_O], in_z.at[gs_slot, 0], 1, "rs", 1, gs_key, peer(2, 1))

    text_grad = window(own_text, iw, text_grad)
    text_unit = t_ref[...].astype(F32) / text_length
    along = jnp.sum(text_unit * text_grad, axis=1, keepdims=True)
    gt_ref[...] = ((text_grad - text_unit * along) / text_length).astype(BF)

    @pl.when(lead)
    def _():
        total = base(0, "o", FULL)
        for i, key in enumerate(("g1o", "g2o", "g3o")):
            arrived(in_z.at[i, 0], 1, key)
            total += in_z[i, 0].astype(F32)
        pre_out[...] = total[0]
        send(pre_out, pre_in, 1, "pre", 0, "pre", partner)
        pre_in[...] = total[1]
        arrived(in_fin, 1, "fin")

    @pl.when(hub)
    def _():
        arrived(pre_in, 0, "pre")
        arrived(in_fin, 0, "fin")

    gw_ref[...] = pre_in[...] + in_fin[0].astype(F32) + in_fin[1].astype(F32)

    tw.drain()
    iw.drain()

    @pl.when(hub)
    def _():
        drained(shards(6), 0, "ag")
        drained(shards(n), 0, "g0")

    @pl.when(lead)
    def _():
        drained(shards(25), 1, "ag")
        drained(shards(n - 1), 1, "w")
        drained(shards(30), 1, "rs")
        drained(pre_out, 1, "pre")

    assert max(map(len, sends)) <= SENDS
    assert max(map(len, recvs)) <= RECVS


def fused(n, axis, image_features, head_weight, text_embeds, factor, bias):
    rows, width = image_features.shape
    own_rows, cols = head_weight.shape
    hbm = pl.BlockSpec(memory_space=pltpu.HBM)
    vmem = pl.BlockSpec(memory_space=pltpu.VMEM)
    two = (2, own_rows, cols)
    scratch = [
        ((rows, width), BF),
        ((rows, cols), BF),
        ((n, own_rows, cols), BF),
        ((rows, cols), BF),
        ((5, rows, cols), BF),
        ((rows, cols), BF),
        ((5, rows, cols), BF),
        ((width, rows), BF),
        ((4, 4) + two, F32),
        ((4, 4) + two, BF),
        ((4, 4) + two, BF),
        ((4, 4) + two, BF),
        ((4,) + two, BF),
        ((2,) + two, BF),
        ((3, 3) + two, BF),
        ((2,) + two, BF),
        (two, BF),
        ((own_rows, cols), F32),
        ((own_rows, cols), F32),
        ((rows, cols), F32),
    ]
    shapes = (((rows, width), BF), ((rows, cols), BF), ((own_rows, cols), F32))
    results = pl.pallas_call(
        functools.partial(kernel, n, axis),
        out_shape=tuple(pltpu.VMEM(s, d) for s, d in shapes),
        in_specs=[hbm] * 5,
        out_specs=(vmem, vmem, vmem),
        scratch_shapes=[pltpu.VMEM(s, d) for s, d in scratch]
        + [pltpu.SMEM((1,), F32)] * 2
        + [pltpu.SemaphoreType.DMA((k,)) for k in (5, SENDS, RECVS)]
        + [pltpu.SemaphoreType.REGULAR],
        compiler_params=pltpu.CompilerParams(
            collective_id=0, has_side_effects=True, vmem_limit_bytes=65413120
        ),
    )(image_features, head_weight, text_embeds, factor, bias)
    return pl.pallas_call(
        write_out,
        out_shape=tuple(jax.ShapeDtypeStruct(s, d) for s, d in shapes),
        in_specs=[vmem] * 3,
        out_specs=(hbm,) * 3,
        scratch_shapes=[pltpu.SemaphoreType.DMA((3,))],
        compiler_params=pltpu.CompilerParams(vmem_limit_bytes=2**20),
    )(*results)


def write_out(gx, gt, gw, gx_out, gt_out, gw_out, sems):
    pairs = ((gx, gx_out), (gt, gt_out), (gw, gw_out))
    copies = [pltpu.make_async_copy(a, b, sems.at[i]) for i, (a, b) in enumerate(pairs)]
    for c in copies:
        c.start()
    for c in copies:
        c.wait()


def passed_along(block, axis, distance):
    devices = range(lax.axis_size(axis))
    route = [((i - distance) % len(devices), i) for i in devices]
    return lax.ppermute(block, axis, route)


def normalize(rows):
    squares = jnp.sum(rows * rows, axis=1, keepdims=True)
    length = jnp.sqrt(squares + epsilon)
    return (rows / length, length)


def similarity_derivative(
    picture_sample_group,
    caption_sample_group,
    similarity_multiplier,
    neighbour_distance,
    outer_dimension_size,
):
    similarity_matrix = (
        similarity_multiplier
        * lax.dot_general(
            picture_sample_group,
            caption_sample_group,
            (((1,), (1,)), ((), ())),
            preferred_element_type=jnp.float32,
        )
        + neighbour_distance
    )
    if outer_dimension_size:
        matched = lax.broadcasted_iota(
            jnp.int32, similarity_matrix.shape, 0
        ) == lax.broadcasted_iota(jnp.int32, similarity_matrix.shape, 1)
        match_polarity = jnp.where(matched, 1.0, -1.0).astype(jnp.float32)
    else:
        match_polarity = -jnp.ones(similarity_matrix.shape, jnp.float32)
    return (
        -similarity_multiplier
        * match_polarity
        * jax.nn.sigmoid(-match_polarity * similarity_matrix)
    ).astype(jnp.bfloat16)


def project_back(grad, unit_rows, length):
    return (grad - unit_rows * jnp.sum(unit_rows * grad, axis=1, keepdims=True)) / length


def by_collectives(image_features, head_weight, text_embeds, natural_exponent_factor, logit_bias):
    full_weight = lax.all_gather(head_weight, "blk", axis=0, tiled=True)
    embedded = jnp.dot(image_features, full_weight, preferred_element_type=jnp.float32)
    image_unit, image_length = normalize(embedded)
    picture_embedding_mapped = image_unit.astype(jnp.bfloat16)
    text_unit, text_length = normalize(text_embeds.astype(jnp.float32))
    text_low = text_unit.astype(jnp.bfloat16)
    similarity_multiplier = jnp.exp(natural_exponent_factor[0])
    neighbour_distance = logit_bias[0]
    image_grad = jnp.zeros(image_unit.shape, jnp.float32)
    current_neighbour_tile = text_low
    for partition_portion in range(S):
        mapping_matrix = similarity_derivative(
            picture_embedding_mapped,
            current_neighbour_tile,
            similarity_multiplier,
            neighbour_distance,
            partition_portion == 0,
        )
        image_grad = image_grad + jnp.dot(
            mapping_matrix, current_neighbour_tile, preferred_element_type=jnp.float32
        )
        if partition_portion + 1 < S:
            current_neighbour_tile = passed_along(current_neighbour_tile, "blk", -1)
    text_grad = jnp.zeros(text_unit.shape, jnp.float32)
    passing = picture_embedding_mapped
    for partition_portion in range(S):
        mapping_matrix = similarity_derivative(
            passing, text_low, similarity_multiplier, neighbour_distance, partition_portion == 0
        )
        text_grad = text_grad + lax.dot_general(
            mapping_matrix, passing, (((0,), (0,)), ((), ())), preferred_element_type=jnp.float32
        )
        if partition_portion + 1 < S:
            passing = passed_along(passing, "blk", 1)
    embed_grad = project_back(image_grad, image_unit, image_length).astype(jnp.bfloat16)
    grad_text = project_back(text_grad, text_unit, text_length).astype(jnp.bfloat16)
    grad_features = lax.dot_general(
        embed_grad, full_weight, (((1,), (1,)), ((), ())), preferred_element_type=jnp.float32
    ).astype(jnp.bfloat16)
    grad_weight = lax.psum_scatter(
        lax.dot_general(
            image_features, embed_grad, (((0,), (0,)), ((), ())), preferred_element_type=jnp.float32
        ),
        "blk",
        scatter_dimension=0,
        tiled=True,
    )
    return (grad_features, grad_text, grad_weight)


def on_device(image_features, head_weight, text_embeds, natural_exponent_factor, logit_bias):
    n = lax.axis_size("blk")
    whole_tiles = head_weight.shape[0] % 16 == 0 and n % 8 == 0 and n // 8 == 4
    run = functools.partial(fused, n, "blk") if whole_tiles else by_collectives
    return run(image_features, head_weight, text_embeds, natural_exponent_factor, logit_bias)


def solution(mesh):
    return jax.shard_map(
        on_device,
        mesh=mesh,
        in_specs=(P("blk", None), P("blk", None), P("blk", None), P(), P()),
        out_specs=(P("blk", None), P("blk", None), P("blk", None)),
        check_vma=False,
    )
```

```python
import functools

import jax
import jax.numpy as jnp
from jax import lax
from jax.experimental import pallas as pl
from jax.experimental.pallas import tpu as pltpu
from jax.sharding import PartitionSpec as P

S = 4
epsilon = 1e-06
MESH = pl.DeviceIdType.MESH
F32 = jnp.float32
BF = jnp.bfloat16


def dot_nt(a, b):
    return lax.dot_general(a, b, (((1,), (1,)), ((), ())), preferred_element_type=F32)


def pair_grad(rows, cols, t, bias, own):
    logits = t * dot_nt(rows, cols) + bias
    if own:
        matched = lax.broadcasted_iota(jnp.int32, logits.shape, 0) == lax.broadcasted_iota(
            jnp.int32, logits.shape, 1
        )
        z = jnp.where(matched, 1.0, -1.0).astype(F32)
        return (-t * z * jax.nn.sigmoid(-z * logits)).astype(BF)
    return (t * jax.nn.sigmoid(logits)).astype(BF)


CHUNKS = 4
SENDS = 16
RECVS = 48


class Keys(dict):
    def __missing__(self, key):
        self[key] = len(self)
        return self[key]


def kernel(
    n, axis,
    x_hbm, w_hbm, t_hbm, lf_hbm, bias_hbm,
    gx_ref, gt_ref, gw_ref,
    x_ref, t_ref, w_all, text_low, text_in, image_low, image_in, xt, gz, from_core, to_core,
    out_s, in_d, in_xy, in_z, in_e, in_fin, pre_out, pre_in, embedded_ref,
    factor_ref, bias_ref, load_sem, send_sem, recv_sem, credit,
):
    rows, width = x_ref.shape
    own_rows, cols = w_all.shape[1:]
    ha = (cols // 128 + 1) // 2 * 128
    A, B, FULL = pl.ds(0, ha), pl.ds(ha, cols - ha), pl.ds(0, cols)
    me = lax.axis_index(axis)
    core = lax.rem(me, 2)
    chip = me // 2
    x = lax.rem(chip, 2)
    y = lax.rem(chip // 2, 2)
    z = chip // 4
    side = z // 2
    plane = [z, z + 1 - 2 * lax.rem(z, 2), 2 - side, 3 * (1 - side)]
    inner = lax.rem(z + side, 2) == 1
    outer = jnp.logical_not(inner)
    hub = core == 0
    lead = core == 1
    sends = (Keys(), Keys())
    recvs = (Keys(), Keys())

    def dev(z_, y_, x_, c_):
        return ((z_ * 2 + y_) * 2 + x_) * 2 + c_

    def xn(c_):
        return dev(z, y, 1 - x, c_)

    def yn(c_):
        return dev(z, 1 - y, x, c_)

    def peer(p, c_):
        return dev(plane[p], y, x, c_)

    partner = dev(z, y, x, 1 - core)

    def send(src, dst, role, key, to_role, recv, target, cond=None):
        c = pltpu.make_async_remote_copy(
            src_ref=src, dst_ref=dst, send_sem=send_sem.at[sends[role][key]],
            recv_sem=recv_sem.at[recv if not isinstance(recv, (str, tuple)) else recvs[to_role][recv]],
            device_id=(target,), device_id_type=MESH,
        )
        if cond is None:
            c.start()
        else:
            pl.when(cond)(c.start)

    def arrived(ref, role, key):
        pltpu.make_async_remote_copy(
            src_ref=ref, dst_ref=ref, send_sem=send_sem.at[0],
            recv_sem=recv_sem.at[recvs[role][key]],
            device_id=(partner,), device_id_type=MESH,
        ).wait_recv()

    def drained(ref, role, key):
        pltpu.make_async_remote_copy(
            src_ref=ref, dst_ref=ref, send_sem=send_sem.at[sends[role][key]],
            recv_sem=recv_sem.at[0], device_id=(partner,), device_id_type=MESH,
        ).wait_send()

    def shards(count):
        return w_all.at[pl.ds(0, count)]

    barrier = pltpu.get_barrier_semaphore()
    peers = [partner]
    for c in range(2):
        peers += [xn(c), yn(c)] + [peer(p, c) for p in range(1, 4)]
    peers += [lax.rem(me + n + s, n) for s in (-2, 2, -4, 4)]
    for p in peers:
        pl.semaphore_signal(barrier, inc=1, device_id=(p,), device_id_type=MESH)

    pairs = [
        (w_hbm, w_all.at[me]), (t_hbm, t_ref), (lf_hbm, factor_ref), (bias_hbm, bias_ref),
        (x_hbm, x_ref),
    ]
    loads = [pltpu.make_async_copy(a, b, load_sem.at[i]) for i, (a, b) in enumerate(pairs)]
    for c in loads:
        c.start()
    loads[0].wait()

    pl.semaphore_wait(barrier, len(peers))

    part = rows // CHUNKS

    def cut_rows(c):
        return pl.ds(c * part, part)

    class Window:
        def __init__(self, key, buf, slots, mirror):
            self.key, self.buf, self.slots, self.mirror = key, buf, slots, mirror
            v = n - 1 - me if mirror else me
            q = lax.rem(v // 2, 4)
            step = 2 if mirror else -2
            back = lax.rem(me + n + step, n)
            back2 = lax.rem(me + n + 2 * step, n)
            self.back = back
            odd = lax.rem(q, 2) == 1
            even = jnp.logical_not(odd)
            self.odd, self.even, self.back2 = odd, even, back2
            self.leaf_third = 2 if mirror else 3
            self.low, self.high = slots.at[2], buf
            if not mirror:
                self.low, self.high = buf, slots.at[2]

        def at(self, slot, c):
            return self.slots.at[slot, cut_rows(c)]

        def leaf_sends(self):
            send(self.buf, self.slots.at[2], 1, (self.key, "own"), 0, (self.key, "own"), partner)

        def hub_own(self):
            send(self.buf, self.slots.at[2], 0, (self.key, "all"), 1, (self.key, "third"), partner)

        def wait_own(self):
            arrived(self.slots.at[2], 0, (self.key, "own"))

        def start_low(self, c):
            r = cut_rows(c)
            send(
                self.low.at[r], self.at(3, c), 0, (self.key, "all"), 0,
                (self.key, 3, c), self.back2,
            )
            send(
                self.low.at[r], self.at(0, c), 0, (self.key, "mixed"), 0,
                (self.key, 0, c), self.back, self.odd,
            )

        def start_high(self, c):
            r = cut_rows(c)
            send(
                self.high.at[r], self.at(1, c), 0, (self.key, "all"), 0,
                (self.key, 1, c), self.back,
            )

        def far(self, c):
            arrived(self.at(3, c), 0, (self.key, 3, c))
            send(
                self.at(3, c), self.at(0, c), 0, (self.key, "mixed"), 0,
                (self.key, 0, c), xn(0), self.even,
            )
            if not self.mirror:
                send(
                    self.at(3, c), self.at(3, c), 0, (self.key, "all"), 1,
                    (self.key, "third"), partner,
                )

        def near(self, slot, c):
            arrived(self.at(slot, c), 0, (self.key, slot, c))
            send(
                self.at(slot, c), self.at(slot, c), 0, (self.key, "all"), 1,
                (self.key, slot), partner,
            )

        def third(self):
            return 3 - core if self.mirror else 2 + core

        def leaf_wait(self, slot):
            arrived(self.slots.at[slot], 1, (self.key, slot if slot < 2 else "third"))

        def drain(self):
            @pl.when(hub)
            def _():
                drained(self.slots, 0, (self.key, "all"))
                drained(self.slots.at[0], 0, (self.key, "mixed"))

            @pl.when(lead)
            def _():
                drained(self.slots.at[0], 1, (self.key, "own"))

    def release():
        pl.semaphore_signal(credit, inc=1, device_id=(partner,), device_id_type=MESH)

    tw = Window("t", text_low, text_in, False)
    iw = Window("i", image_low, image_in, True)

    def place(r):
        return (y, 1 - y)[r in ("y", "d")], (x, 1 - x)[r in ("x", "d")]

    def pair(p, r, cut=FULL):
        y_, x_ = place(r)
        return w_all.at[pl.ds(pl.multiple_of(dev(plane[p], y_, x_, 0), 2), 2), :, cut]

    for key in ("o1", "o2", "o3", "px0", "py0"):
        recvs[1][key]
    far_key = jnp.where(inner, recvs[1]["o2"], recvs[1]["o3"])
    own = w_all.at[me]

    def wait_pair(p, r, key):
        arrived(pair(p, r), 1, key)
        send(pair(p, r), pair(p, r), 1, "w", 0, ("w", p), partner)

    def onto(p, r, cut, recv, target, key="ag", cond=None):
        send(pair(p, r, cut), pair(p, r, cut), 1, key, 1, recv, target, cond)

    def diagonal(p):
        wait_pair(p, "d", ("d", p))

    def side_x(p, key):
        arrived(pair(p, "x"), 1, key)
        onto(p, "x", A, ("d", p), yn(1))

    def side_y(p, key):
        arrived(pair(p, "y"), 1, key)
        onto(p, "y", B, ("d", p), xn(1))

    def swap(p, r):
        send(pair(p, r), pair(p, r), 1, "w", 0, ("w", p), partner)

    def first_sends(role):
        for target, recv in (
            (peer(3, 1), far_key), (peer(2, 1), far_key), (peer(1, 1), "o1"),
            (xn(1), "px0"), (yn(1), "py0"),
        ):
            send(own, own, role, "ag", 1, recv, target)

    @pl.when(hub)
    def _():
        first_sends(0)
        send(own, own, 0, "ag", 1, "w0", partner)

    @pl.when(lead)
    def _():
        first_sends(1)
        send(own, own, 1, "w", 0, ("w", 0), partner)

    for c in loads[1:4]:
        c.wait()
    t = jnp.exp(jnp.full((1, 1), factor_ref[0], F32))
    bias = bias_ref[0]
    text = t_ref[...].astype(F32)
    text_length = jnp.sqrt(jnp.sum(text * text, axis=1, keepdims=True) + epsilon)
    text_low[...] = (text / text_length).astype(BF)

    @pl.when(hub)
    def _():
        tw.start_low(0)
        tw.wait_own()
        tw.start_high(0)
        pl.semaphore_wait(credit, 1)
        tw.start_low(1)
        tw.start_high(1)
        tw.far(0)
        pl.semaphore_wait(credit, 1)
        tw.start_low(2)
        tw.start_high(2)
        tw.far(1)
        pl.semaphore_wait(credit, 1)
        tw.start_low(3)
        tw.start_high(3)
        tw.far(2)
        tw.far(3)

    @pl.when(lead)
    def _():
        tw.leaf_sends()

        side_x(0, "px0")
        onto(0, "x", FULL, ("zx", 1), peer(1, 1))
        onto(0, "x", FULL, ("zx", 2), peer(2, 1), "ag", inner)
        swap(0, "x")
        side_y(0, "py0")
        onto(0, "y", FULL, ("zy", 1), peer(1, 1))
        onto(0, "y", FULL, ("zy", 2), peer(2, 1), "ag", inner)
        swap(0, "y")
        arrived(pair(3, "o"), 1, "o3")
        onto(3, "o", FULL, "px3", xn(1))
        onto(3, "o", FULL, "py3", yn(1))
        swap(3, "o")
        arrived(pair(2, "o"), 1, "o2")
        onto(2, "o", FULL, ("zx", 2), xn(1), "ag", outer)
        onto(2, "o", FULL, ("zy", 2), yn(1), "ag", outer)
        swap(2, "o")
        wait_pair(1, "o", "o1")
        release()
        diagonal(0)
        side_x(1, ("zx", 1))
        swap(1, "x")
        side_y(1, ("zy", 1))
        swap(1, "y")
        release()
        side_x(3, "px3")
        swap(3, "x")
        side_y(3, "py3")
        swap(3, "y")
        release()
        side_x(2, ("zx", 2))
        swap(2, "x")
        side_y(2, ("zy", 2))
        swap(2, "y")
        diagonal(1)

    loads[4].wait()
    xt[...] = x_ref[...].T

    @pl.when(hub)
    def _():
        arrived(shards(7), 0, ("w", 0))
        arrived(shards(8), 0, ("w", 1))

    def project(p):
        at = pl.ds(pl.multiple_of(plane[p] * 8 * own_rows, 8 * own_rows), 8 * own_rows)
        rows_of = w_all[pl.ds(pl.multiple_of(plane[p] * 8, 8), 8)].reshape(8 * own_rows, cols)
        return jnp.dot(x_ref[:, at], rows_of, preferred_element_type=F32)

    @pl.when(lead)
    def _():
        arrived(w_all.at[partner], 1, "w0")

    embedded_ref[...] = project(0)
    embedded_ref[...] += project(1)

    @pl.when(hub)
    def _():
        for c in range(CHUNKS):
            tw.near(1, c)
        arrived(shards(8), 0, ("w", 3))

    @pl.when(lead)
    def _():
        diagonal(3)

    embedded_ref[...] += project(3)

    @pl.when(hub)
    def _():
        for c in range(CHUNKS):
            tw.near(0, c)
        arrived(shards(8), 0, ("w", 2))

    @pl.when(lead)
    def _():
        diagonal(2)

    weight = w_all[...].reshape(n * own_rows, cols)
    embedded = embedded_ref[...] + project(2)
    image_length = jnp.sqrt(jnp.sum(embedded * embedded, axis=1, keepdims=True) + epsilon)
    image_unit = embedded / image_length
    image_low[...] = image_unit.astype(BF)

    @pl.when(hub)
    def _():
        iw.hub_own()
        iw.start_high(0)
        iw.start_high(1)

    @pl.when(lead)
    def _():
        iw.leaf_sends()

    mine = image_low[...]
    own_text = text_low[...]
    grad = pair_grad(mine, own_text, t, bias, True)
    image_grad = jnp.dot(grad, own_text, preferred_element_type=F32)

    @pl.when(hub)
    def _():
        iw.wait_own()
        iw.start_low(0)
        iw.start_low(1)
        iw.start_low(2)
        iw.start_low(3)

    def window(low, win, grads):
        for i, q in enumerate((win.third(), 1, 0)):
            @pl.when(lead)
            def _():
                win.leaf_wait((win.leaf_third, 1, 0)[i])

            block = win.slots[q]
            grads += jnp.dot(
                pair_grad(low, block, t, bias, False), block, preferred_element_type=F32
            )
        return grads

    image_grad = window(mine, tw, image_grad)
    along = jnp.sum(image_unit * image_grad, axis=1, keepdims=True)
    embed_grad = ((image_grad - image_unit * along) / image_length).astype(BF)

    def hand_over(p, r):
        y_, x_ = place(r)
        c = y_ * 2 + x_
        key = ("g0", p, "d" if r == "d" else "rest")
        send(to_core.at[p, c], from_core.at[p, c], 0, "g0", 1, key, partner)

    group = 8 * own_rows
    for p in (3, 2, 1, 0):
        lhs = xt[pl.ds(pl.multiple_of(plane[p] * group, group), group), :]
        product = jnp.dot(lhs, embed_grad, preferred_element_type=F32)
        gz[p] = product.reshape(4, 2, own_rows, cols)

        @pl.when(hub)
        def _():
            to_core[p] = gz[p].astype(BF)
            hand_over(p, "d")

    @pl.when(hub)
    def _():
        for p in (3, 2, 1, 0):
            for r in ("x", "y", "o"):
                hand_over(p, r)

    S_O, S_X, S_Y, S_D = range(4)

    def base(p, r, cut):
        y_, x_ = place(r)
        c = y_ * 2 + x_
        return gz[p, c, :, :, cut] + from_core[p, c, :, :, cut].astype(F32)

    def put(p, r, cut, value):
        out_s[p, r, :, :, cut] = value.astype(BF)

    def open_plane(p):
        arrived(from_core.at[p, 0], 1, ("g0", p, "d"))
        put(p, S_D, FULL, base(p, "d", FULL))
        send(out_s.at[p, S_D, :, :, A], in_d.at[p, :, :, A], 1, "rs", 1, ("gd", p), yn(1))
        send(out_s.at[p, S_D, :, :, B], in_d.at[p, :, :, B], 1, "rs", 1, ("gd", p), xn(1))

    for key in ("g1o", "g2o", "g3o"):
        recvs[1][key]
    gs_key = jnp.where(inner, recvs[1]["g2o"], recvs[1]["g3o"])
    gs_slot = jnp.where(inner, 1, 2)

    def rest(p):
        arrived(from_core.at[p, pl.ds(0, 3)], 1, ("g0", p, "rest"))

    def sides(p):
        arrived(in_d.at[p], 1, ("gd", p))

    def x_sum(p, cut):
        v = base(p, "x", cut)
        return v + in_d[p, :, :, cut].astype(F32) if cut is A else v

    def y_sum(p, cut):
        v = base(p, "y", cut)
        return v + in_d[p, :, :, cut].astype(F32) if cut is B else v

    def put_sides(p, first):
        cx, cy = (B, A) if first else (A, B)
        put(p, S_X, cx, x_sum(p, cx))
        put(p, S_Y, cy, y_sum(p, cy))

    def send_sides(p, first, buf, i, key, tx, ty):
        cx, cy = (B, A) if first else (A, B)
        for r, cut, target in ((0, cx, tx), (1, cy, ty)):
            dst = buf.at[r, :, :, cut] if i is None else buf.at[i, r + 1, :, :, cut]
            send(out_s.at[p, S_X + r, :, :, cut], dst, 1, "rs", 1, key, target)

    def sides_of(p, first):
        if not first:
            sides(p)
        put_sides(p, first)
        if p == 3:
            send_sides(p, first, in_xy, None, "gxy3", xn(1), yn(1))
        if p == 1:
            send_sides(p, first, in_z, 0, "g1xy", peer(1, 1), peer(1, 1))
        if p == 2:
            @pl.when(outer)
            def _():
                send_sides(p, first, in_e, None, "ge", xn(1), yn(1))

            @pl.when(inner)
            def _():
                send_sides(p, first, in_z, 1, "g2xy", peer(2, 1), peer(2, 1))

    gx_ref[...] = dot_nt(embed_grad, weight).astype(BF)

    text_grad = jnp.dot(
        pair_grad(own_text, mine, t, bias, True), mine, preferred_element_type=F32
    )

    @pl.when(lead)
    def _():
        open_plane(3)
        open_plane(2)
        open_plane(1)
        rest(3)
        sides_of(3, True)
        rest(2)

        @pl.when(inner)
        def _():
            put(2, S_O, FULL, base(2, "o", FULL))
            send(out_s.at[2, S_O], in_z.at[gs_slot, 0], 1, "rs", 1, gs_key, peer(2, 1))

        sides_of(2, True)
        rest(1)
        put(1, S_O, FULL, base(1, "o", FULL))
        send(out_s.at[1, S_O], in_z.at[0, 0], 1, "rs", 1, "g1o", peer(1, 1))
        sides_of(1, True)
        sides_of(3, False)
        release()
        open_plane(0)
        rest(0)

    @pl.when(hub)
    def _():
        iw.far(0)
        iw.far(1)
        iw.far(2)
        pl.semaphore_wait(credit, 1)
        iw.start_high(2)
        iw.start_high(3)
        iw.far(3)
        for c in range(CHUNKS):
            iw.near(1, c)
        for c in range(CHUNKS):
            iw.near(0, c)

    @pl.when(lead)
    def _():
        sides_of(2, False)
        sides_of(1, False)

    @pl.when(lead)
    def _():
        arrived(in_xy, 1, "gxy3")
        put(
            3, S_O, FULL,
            base(3, "o", FULL) + in_xy[0].astype(F32) + in_xy[1].astype(F32),
        )
        send(out_s.at[3, S_O], in_z.at[gs_slot, 0], 1, "rs", 1, gs_key, peer(3, 1))

    @pl.when(lead)
    def _():
        sides(0)
        arrived(in_z.at[0, pl.ds(1, 2)], 1, "g1xy")


        @pl.when(outer)
        def _():
            for cut in (A, B):
                put(0, S_X, cut, x_sum(0, cut) + in_z[0, 1, :, :, cut].astype(F32))
                put(0, S_Y, cut, y_sum(0, cut) + in_z[0, 2, :, :, cut].astype(F32))

        @pl.when(inner)
        def _():
            arrived(in_z.at[1, pl.ds(1, 2)], 1, "g2xy")
            for cut in (A, B):
                for r, fill in ((1, x_sum), (2, y_sum)):
                    put(
                        0, r, cut,
                        fill(0, cut) + in_z[0, r, :, :, cut].astype(F32)
                        + in_z[1, r, :, :, cut].astype(F32),
                    )

        for c in range(2):
            send(out_s.at[0, S_X, c], in_fin.at[0], 1, "rs", c, "fin", xn(c))
            send(out_s.at[0, S_Y, c], in_fin.at[1], 1, "rs", c, "fin", yn(c))

        @pl.when(outer)
        def _():
            arrived(in_e, 1, "ge")
            put(
                2, S_O, FULL,
                base(2, "o", FULL) + in_e[0].astype(F32) + in_e[1].astype(F32),
            )
            send(out_s.at[2, S_O], in_z.at[gs_slot, 0], 1, "rs", 1, gs_key, peer(2, 1))

    text_grad = window(own_text, iw, text_grad)
    text_unit = t_ref[...].astype(F32) / text_length
    along = jnp.sum(text_unit * text_grad, axis=1, keepdims=True)
    gt_ref[...] = ((text_grad - text_unit * along) / text_length).astype(BF)

    @pl.when(lead)
    def _():
        total = base(0, "o", FULL)
        for i, key in enumerate(("g1o", "g2o", "g3o")):
            arrived(in_z.at[i, 0], 1, key)
            total += in_z[i, 0].astype(F32)
        pre_out[...] = total[0]
        send(pre_out, pre_in, 1, "pre", 0, "pre", partner)
        pre_in[...] = total[1]
        arrived(in_fin, 1, "fin")

    @pl.when(hub)
    def _():
        arrived(pre_in, 0, "pre")
        arrived(in_fin, 0, "fin")

    gw_ref[...] = pre_in[...] + in_fin[0].astype(F32) + in_fin[1].astype(F32)

    tw.drain()
    iw.drain()

    @pl.when(hub)
    def _():
        drained(shards(6), 0, "ag")
        drained(shards(n), 0, "g0")

    @pl.when(lead)
    def _():
        drained(shards(25), 1, "ag")
        drained(shards(n - 1), 1, "w")
        drained(shards(30), 1, "rs")
        drained(pre_out, 1, "pre")

    assert max(map(len, sends)) <= SENDS
    assert max(map(len, recvs)) <= RECVS


def fused(n, axis, image_features, head_weight, text_embeds, factor, bias):
    rows, width = image_features.shape
    own_rows, cols = head_weight.shape
    hbm = pl.BlockSpec(memory_space=pltpu.HBM)
    vmem = pl.BlockSpec(memory_space=pltpu.VMEM)
    two = (2, own_rows, cols)
    scratch = [
        ((rows, width), BF),
        ((rows, cols), BF),
        ((n, own_rows, cols), BF),
        ((rows, cols), BF),
        ((5, rows, cols), BF),
        ((rows, cols), BF),
        ((5, rows, cols), BF),
        ((width, rows), BF),
        ((4, 4) + two, F32),
        ((4, 4) + two, BF),
        ((4, 4) + two, BF),
        ((4, 4) + two, BF),
        ((4,) + two, BF),
        ((2,) + two, BF),
        ((3, 3) + two, BF),
        ((2,) + two, BF),
        (two, BF),
        ((own_rows, cols), F32),
        ((own_rows, cols), F32),
        ((rows, cols), F32),
    ]
    shapes = (((rows, width), BF), ((rows, cols), BF), ((own_rows, cols), F32))
    results = pl.pallas_call(
        functools.partial(kernel, n, axis),
        out_shape=tuple(pltpu.VMEM(s, d) for s, d in shapes),
        in_specs=[hbm] * 5,
        out_specs=(vmem, vmem, vmem),
        scratch_shapes=[pltpu.VMEM(s, d) for s, d in scratch]
        + [pltpu.SMEM((1,), F32)] * 2
        + [pltpu.SemaphoreType.DMA((k,)) for k in (5, SENDS, RECVS)]
        + [pltpu.SemaphoreType.REGULAR],
        compiler_params=pltpu.CompilerParams(
            collective_id=0, has_side_effects=True, vmem_limit_bytes=65413120
        ),
    )(image_features, head_weight, text_embeds, factor, bias)
    return pl.pallas_call(
        write_out,
        out_shape=tuple(jax.ShapeDtypeStruct(s, d) for s, d in shapes),
        in_specs=[vmem] * 3,
        out_specs=(hbm,) * 3,
        scratch_shapes=[pltpu.SemaphoreType.DMA((3,))],
        compiler_params=pltpu.CompilerParams(vmem_limit_bytes=2**20),
    )(*results)


def write_out(gx, gt, gw, gx_out, gt_out, gw_out, sems):
    pairs = ((gx, gx_out), (gt, gt_out), (gw, gw_out))
    copies = [pltpu.make_async_copy(a, b, sems.at[i]) for i, (a, b) in enumerate(pairs)]
    for c in copies:
        c.start()
    for c in copies:
        c.wait()


def passed_along(block, axis, distance):
    devices = range(lax.axis_size(axis))
    route = [((i - distance) % len(devices), i) for i in devices]
    return lax.ppermute(block, axis, route)


def normalize(rows):
    squares = jnp.sum(rows * rows, axis=1, keepdims=True)
    length = jnp.sqrt(squares + epsilon)
    return (rows / length, length)


def similarity_derivative(
    picture_sample_group,
    caption_sample_group,
    similarity_multiplier,
    neighbour_distance,
    outer_dimension_size,
):
    similarity_matrix = (
        similarity_multiplier
        * lax.dot_general(
            picture_sample_group,
            caption_sample_group,
            (((1,), (1,)), ((), ())),
            preferred_element_type=jnp.float32,
        )
        + neighbour_distance
    )
    if outer_dimension_size:
        matched = lax.broadcasted_iota(
            jnp.int32, similarity_matrix.shape, 0
        ) == lax.broadcasted_iota(jnp.int32, similarity_matrix.shape, 1)
        match_polarity = jnp.where(matched, 1.0, -1.0).astype(jnp.float32)
    else:
        match_polarity = -jnp.ones(similarity_matrix.shape, jnp.float32)
    return (
        -similarity_multiplier
        * match_polarity
        * jax.nn.sigmoid(-match_polarity * similarity_matrix)
    ).astype(jnp.bfloat16)


def project_back(grad, unit_rows, length):
    return (grad - unit_rows * jnp.sum(unit_rows * grad, axis=1, keepdims=True)) / length


def by_collectives(image_features, head_weight, text_embeds, natural_exponent_factor, logit_bias):
    full_weight = lax.all_gather(head_weight, "blk", axis=0, tiled=True)
    embedded = jnp.dot(image_features, full_weight, preferred_element_type=jnp.float32)
    image_unit, image_length = normalize(embedded)
    picture_embedding_mapped = image_unit.astype(jnp.bfloat16)
    text_unit, text_length = normalize(text_embeds.astype(jnp.float32))
    text_low = text_unit.astype(jnp.bfloat16)
    similarity_multiplier = jnp.exp(natural_exponent_factor[0])
    neighbour_distance = logit_bias[0]
    image_grad = jnp.zeros(image_unit.shape, jnp.float32)
    current_neighbour_tile = text_low
    for partition_portion in range(S):
        mapping_matrix = similarity_derivative(
            picture_embedding_mapped,
            current_neighbour_tile,
            similarity_multiplier,
            neighbour_distance,
            partition_portion == 0,
        )
        image_grad = image_grad + jnp.dot(
            mapping_matrix, current_neighbour_tile, preferred_element_type=jnp.float32
        )
        if partition_portion + 1 < S:
            current_neighbour_tile = passed_along(current_neighbour_tile, "blk", -1)
    text_grad = jnp.zeros(text_unit.shape, jnp.float32)
    passing = picture_embedding_mapped
    for partition_portion in range(S):
        mapping_matrix = similarity_derivative(
            passing, text_low, similarity_multiplier, neighbour_distance, partition_portion == 0
        )
        text_grad = text_grad + lax.dot_general(
            mapping_matrix, passing, (((0,), (0,)), ((), ())), preferred_element_type=jnp.float32
        )
        if partition_portion + 1 < S:
            passing = passed_along(passing, "blk", 1)
    embed_grad = project_back(image_grad, image_unit, image_length).astype(jnp.bfloat16)
    grad_text = project_back(text_grad, text_unit, text_length).astype(jnp.bfloat16)
    grad_features = lax.dot_general(
        embed_grad, full_weight, (((1,), (1,)), ((), ())), preferred_element_type=jnp.float32
    ).astype(jnp.bfloat16)
    grad_weight = lax.psum_scatter(
        lax.dot_general(
            image_features, embed_grad, (((0,), (0,)), ((), ())), preferred_element_type=jnp.float32
        ),
        "blk",
        scatter_dimension=0,
        tiled=True,
    )
    return (grad_features, grad_text, grad_weight)


def on_device(image_features, head_weight, text_embeds, natural_exponent_factor, logit_bias):
    n = lax.axis_size("blk")
    whole_tiles = head_weight.shape[0] % 16 == 0 and n % 8 == 0 and n // 8 == 4
    run = functools.partial(fused, n, "blk") if whole_tiles else by_collectives
    return run(image_features, head_weight, text_embeds, natural_exponent_factor, logit_bias)


def solution(mesh):
    return jax.shard_map(
        on_device,
        mesh=mesh,
        in_specs=(P("blk", None), P("blk", None), P("blk", None), P(), P()),
        out_specs=(P("blk", None), P("blk", None), P("blk", None)),
        check_vma=False,
    )
```

```python
import functools

import jax
import jax.numpy as jnp
from jax import lax
from jax.experimental import pallas as pl
from jax.experimental.pallas import tpu as pltpu
from jax.sharding import PartitionSpec as P

S = 4
epsilon = 1e-06
MESH = pl.DeviceIdType.MESH
F32 = jnp.float32
BF = jnp.bfloat16


def dot_nt(a, b):
    return lax.dot_general(a, b, (((1,), (1,)), ((), ())), preferred_element_type=F32)


def pair_grad(rows, cols, t, bias, own):
    logits = t * dot_nt(rows, cols) + bias
    if own:
        matched = lax.broadcasted_iota(jnp.int32, logits.shape, 0) == lax.broadcasted_iota(
            jnp.int32, logits.shape, 1
        )
        z = jnp.where(matched, 1.0, -1.0).astype(F32)
        return (-t * z * jax.nn.sigmoid(-z * logits)).astype(BF)
    return (t * jax.nn.sigmoid(logits)).astype(BF)


CHUNKS = 4
SENDS = 6
RECVS = 42


class Keys(dict):
    def __missing__(self, key):
        self[key] = len(self)
        return self[key]


def kernel(
    n, axis,
    x_hbm, w_hbm, t_hbm, lf_hbm, bias_hbm,
    gx_ref, gt_ref, gw_ref,
    x_ref, t_ref, w_all, text_low, text_in, image_low, image_in, xt, gz, from_core, to_core,
    out_s, in_d, in_xy, in_z, in_e, in_fin, pre_out, pre_in, embedded_ref,
    factor_ref, bias_ref, load_sem, send_sem, recv_sem, credit,
):
    rows, width = x_ref.shape
    own_rows, cols = w_all.shape[1:]
    ha = (cols // 128 + 1) // 2 * 128
    A, B, FULL = pl.ds(0, ha), pl.ds(ha, cols - ha), pl.ds(0, cols)
    me = lax.axis_index(axis)
    core = lax.rem(me, 2)
    chip = me // 2
    x = lax.rem(chip, 2)
    y = lax.rem(chip // 2, 2)
    z = chip // 4
    side = z // 2
    plane = [z, z + 1 - 2 * lax.rem(z, 2), 2 - side, 3 * (1 - side)]
    inner = lax.rem(z + side, 2) == 1
    outer = jnp.logical_not(inner)
    hub = core == 0
    lead = core == 1
    sends = (Keys(), Keys())
    recvs = (Keys(), Keys())

    def dev(z_, y_, x_, c_):
        return ((z_ * 2 + y_) * 2 + x_) * 2 + c_

    def xn(c_):
        return dev(z, y, 1 - x, c_)

    def yn(c_):
        return dev(z, 1 - y, x, c_)

    def peer(p, c_):
        return dev(plane[p], y, x, c_)

    partner = dev(z, y, x, 1 - core)

    def send(src, dst, role, key, to_role, recv, target, cond=None):
        c = pltpu.make_async_remote_copy(
            src_ref=src, dst_ref=dst, send_sem=send_sem.at[sends[role][key]],
            recv_sem=recv_sem.at[recv if not isinstance(recv, (str, tuple)) else recvs[to_role][recv]],
            device_id=(target,), device_id_type=MESH,
        )
        if cond is None:
            c.start()
        else:
            pl.when(cond)(c.start)

    def arrived(ref, role, key):
        pltpu.make_async_remote_copy(
            src_ref=ref, dst_ref=ref, send_sem=send_sem.at[0],
            recv_sem=recv_sem.at[recvs[role][key]],
            device_id=(partner,), device_id_type=MESH,
        ).wait_recv()

    def drained(ref, role, key):
        pltpu.make_async_remote_copy(
            src_ref=ref, dst_ref=ref, send_sem=send_sem.at[sends[role][key]],
            recv_sem=recv_sem.at[0], device_id=(partner,), device_id_type=MESH,
        ).wait_send()

    def shards(count):
        return w_all.at[pl.ds(0, count)]

    barrier = pltpu.get_barrier_semaphore()
    peers = [partner]
    for c in range(2):
        peers += [xn(c), yn(c)] + [peer(p, c) for p in range(1, 4)]
    peers += [lax.rem(me + n + s, n) for s in (-2, 2, -4, 4)]
    for p in peers:
        pl.semaphore_signal(barrier, inc=1, device_id=(p,), device_id_type=MESH)

    pairs = [
        (w_hbm, w_all.at[me]), (t_hbm, t_ref), (lf_hbm, factor_ref), (bias_hbm, bias_ref),
        (x_hbm, x_ref),
    ]
    loads = [pltpu.make_async_copy(a, b, load_sem.at[i]) for i, (a, b) in enumerate(pairs)]
    for c in loads:
        c.start()
    loads[0].wait()

    pl.semaphore_wait(barrier, len(peers))

    part = rows // CHUNKS

    def cut_rows(c):
        return pl.ds(c * part, part)

    class Window:
        def __init__(self, key, buf, slots, mirror):
            self.key, self.buf, self.slots, self.mirror = key, buf, slots, mirror
            v = n - 1 - me if mirror else me
            q = lax.rem(v // 2, 4)
            step = 2 if mirror else -2
            back = lax.rem(me + n + step, n)
            back2 = lax.rem(me + n + 2 * step, n)
            self.back = back
            odd = lax.rem(q, 2) == 1
            even = jnp.logical_not(odd)
            self.odd, self.even, self.back2 = odd, even, back2
            self.leaf_third = 2 if mirror else 3
            self.low, self.high = slots.at[2], buf
            if not mirror:
                self.low, self.high = buf, slots.at[2]

        def at(self, slot, c):
            return self.slots.at[slot, cut_rows(c)]

        def leaf_sends(self):
            send(self.buf, self.slots.at[2], 1, (self.key, "own"), 0, (self.key, "own"), partner)

        def hub_own(self):
            send(self.buf, self.slots.at[2], 0, (self.key, "all"), 1, (self.key, "third"), partner)

        def wait_own(self):
            arrived(self.slots.at[2], 0, (self.key, "own"))

        def start_low(self, c):
            r = cut_rows(c)
            send(
                self.low.at[r], self.at(3, c), 0, (self.key, "all"), 0,
                (self.key, 3, c), self.back2,
            )
            send(
                self.low.at[r], self.at(0, c), 0, (self.key, "mixed"), 0,
                (self.key, 0, c), self.back, self.odd,
            )

        def start_high(self, c):
            r = cut_rows(c)
            send(
                self.high.at[r], self.at(1, c), 0, (self.key, "all"), 0,
                (self.key, 1, c), self.back,
            )

        def far(self, c):
            arrived(self.at(3, c), 0, (self.key, 3, c))
            send(
                self.at(3, c), self.at(0, c), 0, (self.key, "mixed"), 0,
                (self.key, 0, c), xn(0), self.even,
            )
            if not self.mirror:
                send(
                    self.at(3, c), self.at(3, c), 0, (self.key, "all"), 1,
                    (self.key, "third"), partner,
                )

        def near(self, slot, c):
            arrived(self.at(slot, c), 0, (self.key, slot, c))
            send(
                self.at(slot, c), self.at(slot, c), 0, (self.key, "all"), 1,
                (self.key, slot), partner,
            )

        def third(self):
            return 3 - core if self.mirror else 2 + core

        def leaf_wait(self, slot):
            arrived(self.slots.at[slot], 1, (self.key, slot if slot < 2 else "third"))

        def drain(self):
            @pl.when(hub)
            def _():
                drained(self.slots, 0, (self.key, "all"))
                drained(self.slots.at[0], 0, (self.key, "mixed"))

            @pl.when(lead)
            def _():
                drained(self.slots.at[0], 1, (self.key, "own"))

    def release():
        pl.semaphore_signal(credit, inc=1, device_id=(partner,), device_id_type=MESH)

    tw = Window("t", text_low, text_in, False)
    iw = Window("i", image_low, image_in, True)

    def place(r):
        return (y, 1 - y)[r in ("y", "d")], (x, 1 - x)[r in ("x", "d")]

    def pair(p, r, cut=FULL):
        y_, x_ = place(r)
        return w_all.at[pl.ds(pl.multiple_of(dev(plane[p], y_, x_, 0), 2), 2), :, cut]

    for key in ("o1", "o2", "o3", "px0", "py0"):
        recvs[1][key]
    far_key = jnp.where(inner, recvs[1]["o2"], recvs[1]["o3"])
    own = w_all.at[me]

    def wait_pair(p, r, key):
        arrived(pair(p, r), 1, key)
        send(pair(p, r), pair(p, r), 1, "w", 0, ("w", p), partner)

    def onto(p, r, cut, recv, target, key="ag", cond=None):
        send(pair(p, r, cut), pair(p, r, cut), 1, key, 1, recv, target, cond)

    def diagonal(p):
        wait_pair(p, "d", ("d", p))

    def side_x(p, key):
        arrived(pair(p, "x"), 1, key)
        onto(p, "x", A, ("d", p), yn(1))

    def side_y(p, key):
        arrived(pair(p, "y"), 1, key)
        onto(p, "y", B, ("d", p), xn(1))

    def swap(p, r):
        send(pair(p, r), pair(p, r), 1, "w", 0, ("w", p), partner)

    def first_sends(role):
        for target, recv in (
            (peer(3, 1), far_key), (peer(2, 1), far_key), (peer(1, 1), "o1"),
            (xn(1), "px0"), (yn(1), "py0"),
        ):
            send(own, own, role, "ag", 1, recv, target)

    @pl.when(hub)
    def _():
        first_sends(0)
        send(own, own, 0, "ag", 1, "w0", partner)

    @pl.when(lead)
    def _():
        first_sends(1)
        send(own, own, 1, "w", 0, ("w", 0), partner)

    for c in loads[1:4]:
        c.wait()
    t = jnp.exp(jnp.full((1, 1), factor_ref[0], F32))
    bias = bias_ref[0]
    text = t_ref[...].astype(F32)
    text_length = jnp.sqrt(jnp.sum(text * text, axis=1, keepdims=True) + epsilon)
    text_low[...] = (text / text_length).astype(BF)

    @pl.when(hub)
    def _():
        tw.start_low(0)
        tw.start_low(1)
        tw.wait_own()
        tw.start_high(0)
        pl.semaphore_wait(credit, 1)
        tw.start_low(2)
        tw.start_low(3)
        tw.far(0)
        pl.semaphore_wait(credit, 1)
        tw.start_high(1)
        tw.far(1)
        tw.far(2)
        pl.semaphore_wait(credit, 1)
        tw.start_high(2)
        tw.start_high(3)
        tw.far(3)

    @pl.when(lead)
    def _():
        tw.leaf_sends()

        side_x(0, "px0")
        onto(0, "x", FULL, ("zx", 1), peer(1, 1))
        onto(0, "x", FULL, ("zx", 2), peer(2, 1), "ag", inner)
        swap(0, "x")
        side_y(0, "py0")
        onto(0, "y", FULL, ("zy", 1), peer(1, 1))
        onto(0, "y", FULL, ("zy", 2), peer(2, 1), "ag", inner)
        swap(0, "y")
        release()
        arrived(pair(3, "o"), 1, "o3")
        onto(3, "o", FULL, "px3", xn(1))
        onto(3, "o", FULL, "py3", yn(1))
        swap(3, "o")
        arrived(pair(2, "o"), 1, "o2")
        onto(2, "o", FULL, ("zx", 2), xn(1), "ag", outer)
        onto(2, "o", FULL, ("zy", 2), yn(1), "ag", outer)
        swap(2, "o")
        wait_pair(1, "o", "o1")
        release()
        diagonal(0)
        side_x(1, ("zx", 1))
        swap(1, "x")
        side_y(1, ("zy", 1))
        swap(1, "y")
        release()
        side_x(3, "px3")
        swap(3, "x")
        side_y(3, "py3")
        swap(3, "y")
        side_x(2, ("zx", 2))
        swap(2, "x")
        side_y(2, ("zy", 2))
        swap(2, "y")
        diagonal(1)

    loads[4].wait()
    xt[...] = x_ref[...].T

    @pl.when(hub)
    def _():
        arrived(shards(7), 0, ("w", 0))
        arrived(shards(8), 0, ("w", 1))

    def project(p):
        at = pl.ds(pl.multiple_of(plane[p] * 8 * own_rows, 8 * own_rows), 8 * own_rows)
        rows_of = w_all[pl.ds(pl.multiple_of(plane[p] * 8, 8), 8)].reshape(8 * own_rows, cols)
        return jnp.dot(x_ref[:, at], rows_of, preferred_element_type=F32)

    @pl.when(lead)
    def _():
        arrived(w_all.at[partner], 1, "w0")

    embedded_ref[...] = project(0)
    embedded_ref[...] += project(1)

    @pl.when(hub)
    def _():
        for c in range(CHUNKS):
            tw.near(1, c)
        arrived(shards(8), 0, ("w", 3))

    @pl.when(lead)
    def _():
        diagonal(3)

    embedded_ref[...] += project(3)

    @pl.when(hub)
    def _():
        for c in range(CHUNKS):
            tw.near(0, c)
        arrived(shards(8), 0, ("w", 2))

    @pl.when(lead)
    def _():
        diagonal(2)

    weight = w_all[...].reshape(n * own_rows, cols)
    embedded = embedded_ref[...] + project(2)
    image_length = jnp.sqrt(jnp.sum(embedded * embedded, axis=1, keepdims=True) + epsilon)
    image_unit = embedded / image_length
    image_low[...] = image_unit.astype(BF)

    @pl.when(hub)
    def _():
        iw.hub_own()
        iw.start_high(0)
        iw.start_high(1)

    @pl.when(lead)
    def _():
        iw.leaf_sends()

    mine = image_low[...]
    own_text = text_low[...]
    grad = pair_grad(mine, own_text, t, bias, True)
    image_grad = jnp.dot(grad, own_text, preferred_element_type=F32)

    @pl.when(hub)
    def _():
        iw.wait_own()
        iw.start_low(0)
        iw.start_low(1)
        iw.start_low(2)
        iw.start_low(3)

    def window(low, win, grads):
        for i, q in enumerate((win.third(), 1, 0)):
            @pl.when(lead)
            def _():
                win.leaf_wait((win.leaf_third, 1, 0)[i])

            block = win.slots[q]
            grads += jnp.dot(
                pair_grad(low, block, t, bias, False), block, preferred_element_type=F32
            )
        return grads

    image_grad = window(mine, tw, image_grad)
    along = jnp.sum(image_unit * image_grad, axis=1, keepdims=True)
    embed_grad = ((image_grad - image_unit * along) / image_length).astype(BF)

    def hand_over(p, r):
        y_, x_ = place(r)
        c = y_ * 2 + x_
        key = ("g0", p, "d" if r == "d" else "rest")
        send(to_core.at[p, c], from_core.at[p, c], 0, "g0", 1, key, partner)

    group = 8 * own_rows
    for p in (3, 2, 1, 0):
        lhs = xt[pl.ds(pl.multiple_of(plane[p] * group, group), group), :]
        product = jnp.dot(lhs, embed_grad, preferred_element_type=F32)
        gz[p] = product.reshape(4, 2, own_rows, cols)

        @pl.when(hub)
        def _():
            to_core[p] = gz[p].astype(BF)
            hand_over(p, "d")

    @pl.when(hub)
    def _():
        for p in (3, 2, 1, 0):
            for r in ("x", "y", "o"):
                hand_over(p, r)

    S_O, S_X, S_Y, S_D = range(4)

    def base(p, r, cut):
        y_, x_ = place(r)
        c = y_ * 2 + x_
        return gz[p, c, :, :, cut] + from_core[p, c, :, :, cut].astype(F32)

    def put(p, r, cut, value):
        out_s[p, r, :, :, cut] = value.astype(BF)

    def open_plane(p):
        arrived(from_core.at[p, 0], 1, ("g0", p, "d"))
        put(p, S_D, FULL, base(p, "d", FULL))
        send(out_s.at[p, S_D, :, :, A], in_d.at[p, :, :, A], 1, "rs", 1, ("gd", p), yn(1))
        send(out_s.at[p, S_D, :, :, B], in_d.at[p, :, :, B], 1, "rs", 1, ("gd", p), xn(1))

    for key in ("g1o", "g2o", "g3o"):
        recvs[1][key]
    gs_key = jnp.where(inner, recvs[1]["g2o"], recvs[1]["g3o"])
    gs_slot = jnp.where(inner, 1, 2)

    def rest(p):
        arrived(from_core.at[p, pl.ds(0, 3)], 1, ("g0", p, "rest"))

    def sides(p):
        arrived(in_d.at[p], 1, ("gd", p))

    def x_sum(p, cut):
        v = base(p, "x", cut)
        return v + in_d[p, :, :, cut].astype(F32) if cut is A else v

    def y_sum(p, cut):
        v = base(p, "y", cut)
        return v + in_d[p, :, :, cut].astype(F32) if cut is B else v

    def put_sides(p, first):
        cx, cy = (B, A) if first else (A, B)
        put(p, S_X, cx, x_sum(p, cx))
        put(p, S_Y, cy, y_sum(p, cy))

    def send_sides(p, first, buf, i, key, tx, ty):
        cx, cy = (B, A) if first else (A, B)
        for r, cut, target in ((0, cx, tx), (1, cy, ty)):
            dst = buf.at[r, :, :, cut] if i is None else buf.at[i, r + 1, :, :, cut]
            send(out_s.at[p, S_X + r, :, :, cut], dst, 1, "rs", 1, key, target)

    def sides_of(p, first):
        if not first:
            sides(p)
        put_sides(p, first)
        if p == 3:
            send_sides(p, first, in_xy, None, "gxy3", xn(1), yn(1))
        if p == 1:
            send_sides(p, first, in_z, 0, "g1xy", peer(1, 1), peer(1, 1))
        if p == 2:
            @pl.when(outer)
            def _():
                send_sides(p, first, in_e, None, "ge", xn(1), yn(1))

            @pl.when(inner)
            def _():
                send_sides(p, first, in_z, 1, "g2xy", peer(2, 1), peer(2, 1))

    gx_ref[...] = dot_nt(embed_grad, weight).astype(BF)

    text_grad = jnp.dot(
        pair_grad(own_text, mine, t, bias, True), mine, preferred_element_type=F32
    )

    @pl.when(lead)
    def _():
        open_plane(3)
        open_plane(2)
        open_plane(1)
        rest(3)
        sides_of(3, True)
        rest(2)

        @pl.when(inner)
        def _():
            put(2, S_O, FULL, base(2, "o", FULL))
            send(out_s.at[2, S_O], in_z.at[gs_slot, 0], 1, "rs", 1, gs_key, peer(2, 1))

        sides_of(2, True)
        rest(1)
        put(1, S_O, FULL, base(1, "o", FULL))
        send(out_s.at[1, S_O], in_z.at[0, 0], 1, "rs", 1, "g1o", peer(1, 1))
        sides_of(1, True)
        sides_of(3, False)
        release()
        open_plane(0)
        rest(0)

    @pl.when(hub)
    def _():
        iw.far(0)
        iw.far(1)
        iw.far(2)
        pl.semaphore_wait(credit, 1)
        iw.start_high(2)
        iw.start_high(3)
        iw.far(3)
        for c in range(CHUNKS):
            iw.near(1, c)
        for c in range(CHUNKS):
            iw.near(0, c)

    @pl.when(lead)
    def _():
        sides_of(2, False)
        sides_of(1, False)

    @pl.when(lead)
    def _():
        arrived(in_xy, 1, "gxy3")
        put(
            3, S_O, FULL,
            base(3, "o", FULL) + in_xy[0].astype(F32) + in_xy[1].astype(F32),
        )
        send(out_s.at[3, S_O], in_z.at[gs_slot, 0], 1, "rs", 1, gs_key, peer(3, 1))

    @pl.when(lead)
    def _():
        sides(0)
        arrived(in_z.at[0, pl.ds(1, 2)], 1, "g1xy")


        @pl.when(outer)
        def _():
            for cut in (A, B):
                put(0, S_X, cut, x_sum(0, cut) + in_z[0, 1, :, :, cut].astype(F32))
                put(0, S_Y, cut, y_sum(0, cut) + in_z[0, 2, :, :, cut].astype(F32))

        @pl.when(inner)
        def _():
            arrived(in_z.at[1, pl.ds(1, 2)], 1, "g2xy")
            for cut in (A, B):
                for r, fill in ((1, x_sum), (2, y_sum)):
                    put(
                        0, r, cut,
                        fill(0, cut) + in_z[0, r, :, :, cut].astype(F32)
                        + in_z[1, r, :, :, cut].astype(F32),
                    )

        for c in range(2):
            send(out_s.at[0, S_X, c], in_fin.at[0], 1, "rs", c, "fin", xn(c))
            send(out_s.at[0, S_Y, c], in_fin.at[1], 1, "rs", c, "fin", yn(c))

        @pl.when(outer)
        def _():
            arrived(in_e, 1, "ge")
            put(
                2, S_O, FULL,
                base(2, "o", FULL) + in_e[0].astype(F32) + in_e[1].astype(F32),
            )
            send(out_s.at[2, S_O], in_z.at[gs_slot, 0], 1, "rs", 1, gs_key, peer(2, 1))

    text_grad = window(own_text, iw, text_grad)
    text_unit = t_ref[...].astype(F32) / text_length
    along = jnp.sum(text_unit * text_grad, axis=1, keepdims=True)
    gt_ref[...] = ((text_grad - text_unit * along) / text_length).astype(BF)

    @pl.when(lead)
    def _():
        total = base(0, "o", FULL)
        for i, key in enumerate(("g1o", "g2o", "g3o")):
            arrived(in_z.at[i, 0], 1, key)
            total += in_z[i, 0].astype(F32)
        pre_out[...] = total[0]
        send(pre_out, pre_in, 1, "pre", 0, "pre", partner)
        pre_in[...] = total[1]
        arrived(in_fin, 1, "fin")

    @pl.when(hub)
    def _():
        arrived(pre_in, 0, "pre")
        arrived(in_fin, 0, "fin")

    gw_ref[...] = pre_in[...] + in_fin[0].astype(F32) + in_fin[1].astype(F32)

    tw.drain()
    iw.drain()

    @pl.when(hub)
    def _():
        drained(shards(6), 0, "ag")
        drained(shards(n), 0, "g0")

    @pl.when(lead)
    def _():
        drained(shards(25), 1, "ag")
        drained(shards(n - 1), 1, "w")
        drained(shards(30), 1, "rs")
        drained(pre_out, 1, "pre")

    assert max(map(len, sends)) <= SENDS
    assert max(map(len, recvs)) <= RECVS


def fused(n, axis, image_features, head_weight, text_embeds, factor, bias):
    rows, width = image_features.shape
    own_rows, cols = head_weight.shape
    hbm = pl.BlockSpec(memory_space=pltpu.HBM)
    vmem = pl.BlockSpec(memory_space=pltpu.VMEM)
    two = (2, own_rows, cols)
    scratch = [
        ((rows, width), BF),
        ((rows, cols), BF),
        ((n, own_rows, cols), BF),
        ((rows, cols), BF),
        ((5, rows, cols), BF),
        ((rows, cols), BF),
        ((5, rows, cols), BF),
        ((width, rows), BF),
        ((4, 4) + two, F32),
        ((4, 4) + two, BF),
        ((4, 4) + two, BF),
        ((4, 4) + two, BF),
        ((4,) + two, BF),
        ((2,) + two, BF),
        ((3, 3) + two, BF),
        ((2,) + two, BF),
        (two, BF),
        ((own_rows, cols), F32),
        ((own_rows, cols), F32),
        ((rows, cols), F32),
    ]
    shapes = (((rows, width), BF), ((rows, cols), BF), ((own_rows, cols), F32))
    results = pl.pallas_call(
        functools.partial(kernel, n, axis),
        out_shape=tuple(pltpu.VMEM(s, d) for s, d in shapes),
        in_specs=[hbm] * 5,
        out_specs=(vmem, vmem, vmem),
        scratch_shapes=[pltpu.VMEM(s, d) for s, d in scratch]
        + [pltpu.SMEM((1,), F32)] * 2
        + [pltpu.SemaphoreType.DMA((k,)) for k in (5, SENDS, RECVS)]
        + [pltpu.SemaphoreType.REGULAR],
        compiler_params=pltpu.CompilerParams(
            collective_id=0, has_side_effects=True, vmem_limit_bytes=65413120
        ),
    )(image_features, head_weight, text_embeds, factor, bias)
    return pl.pallas_call(
        write_out,
        out_shape=tuple(jax.ShapeDtypeStruct(s, d) for s, d in shapes),
        in_specs=[vmem] * 3,
        out_specs=(hbm,) * 3,
        scratch_shapes=[pltpu.SemaphoreType.DMA((3,))],
        compiler_params=pltpu.CompilerParams(vmem_limit_bytes=2**20),
    )(*results)


def write_out(gx, gt, gw, gx_out, gt_out, gw_out, sems):
    pairs = ((gx, gx_out), (gt, gt_out), (gw, gw_out))
    copies = [pltpu.make_async_copy(a, b, sems.at[i]) for i, (a, b) in enumerate(pairs)]
    for c in copies:
        c.start()
    for c in copies:
        c.wait()


def passed_along(block, axis, distance):
    devices = range(lax.axis_size(axis))
    route = [((i - distance) % len(devices), i) for i in devices]
    return lax.ppermute(block, axis, route)


def normalize(rows):
    squares = jnp.sum(rows * rows, axis=1, keepdims=True)
    length = jnp.sqrt(squares + epsilon)
    return (rows / length, length)


def similarity_derivative(
    picture_sample_group,
    caption_sample_group,
    similarity_multiplier,
    neighbour_distance,
    outer_dimension_size,
):
    similarity_matrix = (
        similarity_multiplier
        * lax.dot_general(
            picture_sample_group,
            caption_sample_group,
            (((1,), (1,)), ((), ())),
            preferred_element_type=jnp.float32,
        )
        + neighbour_distance
    )
    if outer_dimension_size:
        matched = lax.broadcasted_iota(
            jnp.int32, similarity_matrix.shape, 0
        ) == lax.broadcasted_iota(jnp.int32, similarity_matrix.shape, 1)
        match_polarity = jnp.where(matched, 1.0, -1.0).astype(jnp.float32)
    else:
        match_polarity = -jnp.ones(similarity_matrix.shape, jnp.float32)
    return (
        -similarity_multiplier
        * match_polarity
        * jax.nn.sigmoid(-match_polarity * similarity_matrix)
    ).astype(jnp.bfloat16)


def project_back(grad, unit_rows, length):
    return (grad - unit_rows * jnp.sum(unit_rows * grad, axis=1, keepdims=True)) / length


def by_collectives(image_features, head_weight, text_embeds, natural_exponent_factor, logit_bias):
    full_weight = lax.all_gather(head_weight, "blk", axis=0, tiled=True)
    embedded = jnp.dot(image_features, full_weight, preferred_element_type=jnp.float32)
    image_unit, image_length = normalize(embedded)
    picture_embedding_mapped = image_unit.astype(jnp.bfloat16)
    text_unit, text_length = normalize(text_embeds.astype(jnp.float32))
    text_low = text_unit.astype(jnp.bfloat16)
    similarity_multiplier = jnp.exp(natural_exponent_factor[0])
    neighbour_distance = logit_bias[0]
    image_grad = jnp.zeros(image_unit.shape, jnp.float32)
    current_neighbour_tile = text_low
    for partition_portion in range(S):
        mapping_matrix = similarity_derivative(
            picture_embedding_mapped,
            current_neighbour_tile,
            similarity_multiplier,
            neighbour_distance,
            partition_portion == 0,
        )
        image_grad = image_grad + jnp.dot(
            mapping_matrix, current_neighbour_tile, preferred_element_type=jnp.float32
        )
        if partition_portion + 1 < S:
            current_neighbour_tile = passed_along(current_neighbour_tile, "blk", -1)
    text_grad = jnp.zeros(text_unit.shape, jnp.float32)
    passing = picture_embedding_mapped
    for partition_portion in range(S):
        mapping_matrix = similarity_derivative(
            passing, text_low, similarity_multiplier, neighbour_distance, partition_portion == 0
        )
        text_grad = text_grad + lax.dot_general(
            mapping_matrix, passing, (((0,), (0,)), ((), ())), preferred_element_type=jnp.float32
        )
        if partition_portion + 1 < S:
            passing = passed_along(passing, "blk", 1)
    embed_grad = project_back(image_grad, image_unit, image_length).astype(jnp.bfloat16)
    grad_text = project_back(text_grad, text_unit, text_length).astype(jnp.bfloat16)
    grad_features = lax.dot_general(
        embed_grad, full_weight, (((1,), (1,)), ((), ())), preferred_element_type=jnp.float32
    ).astype(jnp.bfloat16)
    grad_weight = lax.psum_scatter(
        lax.dot_general(
            image_features, embed_grad, (((0,), (0,)), ((), ())), preferred_element_type=jnp.float32
        ),
        "blk",
        scatter_dimension=0,
        tiled=True,
    )
    return (grad_features, grad_text, grad_weight)


def on_device(image_features, head_weight, text_embeds, natural_exponent_factor, logit_bias):
    n = lax.axis_size("blk")
    whole_tiles = head_weight.shape[0] % 16 == 0 and n % 8 == 0 and n // 8 == 4
    run = functools.partial(fused, n, "blk") if whole_tiles else by_collectives
    return run(image_features, head_weight, text_embeds, natural_exponent_factor, logit_bias)


def solution(mesh):
    return jax.shard_map(
        on_device,
        mesh=mesh,
        in_specs=(P("blk", None), P("blk", None), P("blk", None), P(), P()),
        out_specs=(P("blk", None), P("blk", None), P("blk", None)),
        check_vma=False,
    )
```
